256 devices in a mesh: node: 256 (over z, x, y, core).
Axes of the slice: x: 4, y: 4, z: 8, core: 2. Of those that a mesh axis runs over, the one named last changes fastest.
Arguments:
- round_index: int32 [1], replicated, may hold values from 0 to 63
- sample_ids: int32 [256, 8], P('node'), may hold values from 0 to 3
- token_pool: bfloat16 [256, 4, 64, 512], P('node'), may hold values from -20 to 20
- cotangent_pool: bfloat16 [256, 4, 64, 512], P('node'), may hold values from -6 to 6
- weights: bfloat16 [256, 4, 512, 512], P('node'), may hold values from -12 to 12
- residue: bfloat16 [256, 4, 512, 512], P('node'), may hold values from -6 to 6
Outputs:
- new_weights: bfloat16 [256, 4, 512, 512], P('node')
- new_residue: bfloat16 [256, 4, 512, 512], P('node')
- grad_rms: float32 [], replicated
The draws below stay inside these ranges and needn't reach their ends.
All inputs are finite; a program needn't handle non-finite values.
Results may differ from the reference program's by a relative error of at most 0.0065.
Values may be sent and summed in bfloat16 or wider, within the bound.
A program may use at most 128 MiB of HBM per device.

```python
import jax
import jax.numpy as jnp
from jax import lax

HEAD_DIM = 64
D = 512
SEQ = 64
BATCH = 8
POOL = 4
NODES = 256
N_NODE = 256


def draw_weights(key, part):
    shape_all = (NODES, 4, D, D)
    drawn = jax.random.normal(key, shape_all, jnp.float32)
    return jnp.clip(drawn, -12.0, 12.0).astype(jnp.bfloat16)


def draw_token_pool(key, part):
    shape_all = (NODES, POOL, SEQ, D)
    drawn = jax.random.normal(key, shape_all, jnp.float32)
    return jnp.clip(drawn, -20.0, 20.0).astype(jnp.bfloat16)


def draw_cotangent_pool(key, part):
    shape_all = (NODES, POOL, SEQ, D)
    rising = (jnp.arange(NODES, dtype=jnp.float32) / max(NODES - 1, 1)).reshape(NODES, 1, 1, 1)
    drawn = jax.random.normal(key, shape_all, jnp.float32) * 0.5 * jnp.power(3.0, 0.5 * rising)
    return jnp.clip(drawn, -6.0, 6.0).astype(jnp.bfloat16)


def place_ends(values, stream_key, smallest, high):
    longest = values.shape.index(max(values.shape))
    spots = []
    for shift in (0, 1):
        where = [jax.random.randint(jax.random.fold_in(stream_key, axis), (), 0, length) for axis, length in enumerate(values.shape)]
        where[longest] = (where[longest] + shift) % values.shape[longest]
        spots.append(tuple(where))
    return values.at[spots[0]].set(smallest).at[spots[1]].set(high)


def steps_of(stream_key, extent, cuts, smallest, top_value):
    gain, own = 1.0, jax.random.fold_in(stream_key, 6)
    for axis_at, parts in cuts:
        heights = jnp.exp(jax.random.uniform(jax.random.fold_in(own, axis_at), (parts,), jnp.float32, smallest / len(cuts), top_value / len(cuts)))
        gain = gain * jnp.repeat(heights, extent[axis_at] // parts).reshape([-1 if axis == axis_at else 1 for axis in range(len(extent))])
    return gain


def centred(own_key, dims, scale, most, shards=(), held_as=jnp.bfloat16):
    entries = jax.random.normal(own_key, dims, jnp.float32) * scale
    if len(shards) > 0:
        entries = steps_of(own_key, dims, shards, -0.22, 0.18) * entries
    return jnp.clip(entries, min=-most, max=most).astype(held_as)


def setup_inputs(seed: int = 0) -> dict:
    keys = jax.random.split(jax.random.key(seed), 7)
    round_index = jax.random.randint(keys[0], (1,), 0, 64).astype(jnp.int32)
    sample_ids = place_ends(jax.random.randint(keys[1], (NODES, BATCH), 0, POOL), jax.random.fold_in(keys[1], 1), 0, POOL - 1).astype(jnp.int32)
    token_pool = draw_token_pool(jax.random.fold_in(keys[6], 71), 0)
    cotangent_pool = draw_cotangent_pool(jax.random.fold_in(keys[6], 71), 0)
    weights = draw_weights(jax.random.fold_in(keys[6], 71), 0)
    residue = centred(keys[5], (NODES, 4, D, D), 1.0, 6.0, ((0, 256),))
    return {"round_index": round_index, "sample_ids": sample_ids, "token_pool": token_pool, "cotangent_pool": cotangent_pool, "weights": weights, "residue": residue}


epsilon = 1e-06
step_rate = 0.1

def normalize(tokens):
    values = tokens.astype(jnp.float32)
    centered = values - lax.optimization_barrier(jnp.mean(values, -1, keepdims=True))
    variance = lax.optimization_barrier(jnp.mean(centered * centered, -1, keepdims=True))
    return (centered * lax.rsqrt(variance + epsilon)).astype(jnp.bfloat16)

def node_gradient(weights, tokens, cotangent):
    batch_size, seq_len, model_width = tokens.shape
    head_count = model_width // HEAD_DIM
    proj_scale = model_width ** (-0.5)
    head_scale = HEAD_DIM ** (-0.5)
    row_count = batch_size * seq_len
    normed_rows = normalize(tokens).reshape(row_count, model_width)
    grad_rows = cotangent.reshape(row_count, model_width)

    def project(which):
        return (jnp.dot(normed_rows, weights[which], preferred_element_type=jnp.float32) * proj_scale).astype(jnp.bfloat16)

    def to_heads(matrix):
        return matrix.reshape(batch_size, seq_len, head_count, HEAD_DIM).astype(jnp.float32)
    queries = to_heads(project(0))
    key_rows = to_heads(project(1))
    value_rows = to_heads(project(2))
    scores = jnp.einsum('bshe,bthe->bhst', queries, key_rows) * head_scale
    attn_probs = jnp.exp(scores - lax.optimization_barrier(jnp.max(scores, -1, keepdims=True)))
    attn_probs = attn_probs / lax.optimization_barrier(jnp.sum(attn_probs, -1, keepdims=True))
    probs_half = attn_probs.astype(jnp.bfloat16).astype(jnp.float32)
    context = jnp.einsum('bhst,bthe->bshe', probs_half, value_rows).astype(jnp.bfloat16).reshape(row_count, model_width)
    grad_out = jnp.dot(context.T, grad_rows, preferred_element_type=jnp.float32) * proj_scale
    context_grad = (jnp.dot(grad_rows, weights[3].T, preferred_element_type=jnp.float32) * proj_scale).astype(jnp.bfloat16)
    context_heads = to_heads(context_grad)
    probs_grad = jnp.einsum('bshe,bthe->bhst', context_heads, value_rows)
    value_grad = jnp.einsum('bhst,bshe->bthe', probs_half, context_heads).astype(jnp.bfloat16)
    score_grad = (attn_probs * (probs_grad - lax.optimization_barrier(jnp.sum(probs_grad * attn_probs, -1, keepdims=True))) * head_scale).astype(jnp.bfloat16).astype(jnp.float32)
    query_grad = jnp.einsum('bhst,bthe->bshe', score_grad, key_rows).astype(jnp.bfloat16)
    key_grad = jnp.einsum('bhst,bshe->bthe', score_grad, queries).astype(jnp.bfloat16)

    def weight_grad(rows_grad):
        return jnp.dot(normed_rows.T, rows_grad.reshape(row_count, model_width), preferred_element_type=jnp.float32) * proj_scale
    return jnp.stack([weight_grad(query_grad), weight_grad(key_grad), weight_grad(value_grad), grad_out])

def reference(round_index, sample_ids, token_pool, cotangent_pool, weights, residue):

    def per_node(node_index):
        sample_rows = sample_ids[node_index]
        tokens = jnp.take(token_pool[node_index], sample_rows, axis=0)
        cotangent = jnp.take(cotangent_pool[node_index], sample_rows, axis=0)
        gradient = node_gradient(weights[node_index], tokens, cotangent)
        tracked = (residue[node_index].astype(jnp.float32) + gradient).astype(jnp.bfloat16)
        return (tracked, gradient, jnp.sum(gradient * gradient))
    tracked, gradient, squares = lax.map(per_node, jnp.arange(N_NODE, dtype=jnp.int32))
    levels = N_NODE.bit_length() - 1
    offset = jnp.left_shift(jnp.int32(1), round_index[0] % levels)

    def track_node(node_index):
        peer_index = (node_index - offset) % N_NODE
        tracker = 0.5 * (tracked[node_index].astype(jnp.float32) + tracked[peer_index].astype(jnp.float32))
        sent = (weights[node_index].astype(jnp.float32) - step_rate * tracker).astype(jnp.bfloat16)
        return (tracker, sent)
    tracker_all, sent_all = lax.map(track_node, jnp.arange(N_NODE, dtype=jnp.int32))

    def mix_node(node_index):
        peer_index = (node_index - offset) % N_NODE
        tracker = tracker_all[node_index]
        mixed = 0.5 * weights[node_index].astype(jnp.float32) + 0.5 * sent_all[peer_index].astype(jnp.float32) - 0.5 * step_rate * tracker
        return (mixed.astype(jnp.bfloat16), (tracker - gradient[node_index]).astype(jnp.bfloat16))
    new_weights, new_residue = lax.map(mix_node, jnp.arange(N_NODE, dtype=jnp.int32))
    grad_rms = jnp.sqrt(jnp.sum(squares) / (N_NODE * gradient[0].size))
    return (new_weights, new_residue, grad_rms)
```

```python
from functools import partial

import jax
import jax.numpy as jnp
from jax import lax
from jax.experimental import pallas as pl
from jax.experimental.pallas import tpu as pltpu
from jax.sharding import PartitionSpec as P

HEAD_DIM = 64
EPSILON = 1e-06
STEP_RATE = 0.1
ROWS = 128
WINDOW = 4

F32, BF16 = jnp.float32, jnp.bfloat16
VMEM, SMEM, ANY = pltpu.VMEM, pltpu.SMEM, pl.ANY


def dot(a, b, contract):
    return lax.dot_general(a, b, ((contract[:1], contract[1:]), ((), ())), preferred_element_type=F32)


def local_kernel(ids_ref, token_ref, cot_ref, w_ref, left_ref, right_ref, q_s, k_s, v_s, c_s):
    pool, seq, width = token_ref.shape
    rows = pool * seq
    proj_scale = width**-0.5
    head_scale = HEAD_DIM**-0.5
    counts = []
    for image in range(pool):
        n = jnp.int32(0)
        for b in range(ids_ref.shape[1]):
            n = n + (ids_ref[0, b] == image).astype(jnp.int32)
        counts.append(n.astype(F32))

    x = token_ref[...].reshape(rows, width).astype(F32)
    centered = x - jnp.mean(x, -1, keepdims=True)
    variance = jnp.mean(centered * centered, -1, keepdims=True)
    normed = (centered * lax.rsqrt(variance + EPSILON)).astype(BF16)
    left_ref[0] = normed.T
    for which, out in enumerate((q_s, k_s, v_s)):
        out[...] = (dot(normed, w_ref[which], (1, 0)) * proj_scale).astype(BF16)
    cot = cot_ref[...].reshape(rows, width)
    right_ref[3] = cot
    cg = dot(cot, w_ref[3], (1, 1))
    for image in range(pool):
        at = slice(image * seq, (image + 1) * seq)
        c_s[at] = (cg[at] * (proj_scale * counts[image])).astype(BF16)

    pair = 2 * seq
    lane = lax.broadcasted_iota(jnp.int32, (pair, 128), 1) < HEAD_DIM
    near = lax.broadcasted_iota(jnp.int32, (seq, 128), 1) < seq
    zero = jnp.zeros((pair, 128), BF16)
    zero_half = jnp.zeros((seq, 128), BF16)

    def by_head(block):
        return jnp.concatenate([jnp.where(lane, block, zero), jnp.where(lane, zero, block)], 0)

    def packed(block):
        return jnp.where(near, block[:seq], block[seq:])

    def spread(block):
        return jnp.concatenate([jnp.where(near, block, zero_half), jnp.where(near, zero_half, block)], 0)

    for b in range(pool // 2):
        at = slice(b * pair, (b + 1) * pair)
        count = jnp.where(near[:1], counts[2 * b], counts[2 * b + 1])
        for j in range(width // 128):
            cols = slice(j * 128, (j + 1) * 128)
            q, k, v, c = q_s[at, cols], k_s[at, cols], v_s[at, cols], c_s[at, cols]
            kk, vv = by_head(k), by_head(v)
            scores = dot(kk, q, (1, 1)) * head_scale
            grads = dot(vv, c, (1, 1))
            probs, back = [], []
            for h in range(2):
                of_head = slice(h * pair, (h + 1) * pair)
                s = packed(scores[of_head])
                e = jnp.exp(s - jnp.max(s, 0, keepdims=True))
                p = e * (1.0 / jnp.sum(e, 0, keepdims=True))
                g = packed(grads[of_head])
                d = p * (g - jnp.sum(g * p, 0, keepdims=True)) * head_scale
                probs.append(spread(p.astype(BF16)))
                back.append(spread(d.astype(BF16)))
            p_rows, d_rows = jnp.concatenate(probs, 0), jnp.concatenate(back, 0)
            p_cols, d_cols = jnp.concatenate(probs, 1), jnp.concatenate(back, 1)
            left_ref[1, cols, at] = (dot(vv, p_rows, (0, 0)) * count).astype(BF16)
            right_ref[0, at, cols] = dot(d_rows, kk, (0, 0)).astype(BF16)
            right_ref[1, at, cols] = dot(d_cols, by_head(q), (1, 0)).astype(BF16)
            right_ref[2, at, cols] = dot(p_cols, by_head(c), (1, 0)).astype(BF16)


def local_part(sample_ids, tokens, cotangent, weights):
    pool, seq, width = tokens.shape
    rows = pool * seq
    return pl.pallas_call(
        local_kernel,
        out_shape=(
            jax.ShapeDtypeStruct((2, width, rows), BF16),
            jax.ShapeDtypeStruct((4, rows, width), BF16),
        ),
        in_specs=[pl.BlockSpec(memory_space=SMEM)] + [pl.BlockSpec(memory_space=VMEM)] * 3,
        out_specs=(pl.BlockSpec(memory_space=VMEM), pl.BlockSpec(memory_space=VMEM)),
        scratch_shapes=[VMEM((rows, width), BF16)] * 4,
        compiler_params=pltpu.CompilerParams(vmem_limit_bytes=32 << 20),
        cost_estimate=pl.CostEstimate(flops=2 * 4 * rows * width * width, bytes_accessed=4 << 20, transcendentals=rows * width),
        name="local",
    )(sample_ids, tokens, cotangent, weights)


def exchange_kernel(
    sizes,
    distance,
    left_ref,
    right_ref,
    w_hbm,
    r_hbm,
    new_w_hbm,
    new_r_hbm,
    rms_ref,
    w_v,
    r_v,
    grad,
    mine,
    sent,
    got_t,
    got_s,
    out_w,
    out_r,
    square,
    parts,
    w_sem,
    r_sem,
    send_sem,
    recv_sem,
    ow_sem,
    or_sem,
    part_send,
    part_recv,
):
    total = 1
    for size in sizes:
        total *= size
    width = w_hbm.shape[-1]
    per = width // ROWS
    chunks = 4 * per
    proj_scale = width**-0.5
    mutual = (2 * distance) % total == 0
    me = lax.axis_index("node")
    ahead = lax.rem(me + distance, total)
    behind = lax.rem(me + total - distance, total)

    groups = []
    stride = 1
    first = 0
    for size in reversed(sizes):
        place = lax.rem(me // stride, size)
        base = me - place * stride
        others = [base + lax.rem(place + d, size) * stride for d in range(1, size)]
        places = [lax.rem(place + d, size) for d in range(1, size)]
        groups.append((first, size, place, others, places))
        first += size
        stride *= size

    barrier = pltpu.get_barrier_semaphore()
    count = 1
    pl.semaphore_signal(barrier, inc=1, device_id=(behind,), device_id_type=pl.DeviceIdType.MESH)
    for _, size, _, others, _ in groups:
        for other in others:
            pl.semaphore_signal(barrier, inc=1, device_id=(other,), device_id_type=pl.DeviceIdType.MESH)
            count += 1

    def at(chunk):
        return chunk // per, pl.ds(pl.multiple_of(lax.rem(chunk, per) * ROWS, ROWS), ROWS)

    def load_r(chunk):
        m, rows = at(chunk)
        return pltpu.make_async_copy(r_hbm.at[m, rows], r_v.at[m, rows], r_sem.at[chunk])

    def load_w(m):
        return pltpu.make_async_copy(w_hbm.at[m], w_v.at[m], w_sem.at[m])

    for chunk in range(chunks):
        load_r(jnp.int32(chunk)).start()
    for m in range(4):
        load_w(m).start()

    square[...] = jnp.zeros_like(square)

    def compute(chunk):
        m, rows = at(chunk)
        g = dot(left_ref[m // 3, rows, :], right_ref[m], (1, 0)) * proj_scale
        load_r(chunk).wait()
        grad[m, rows, :] = g
        mine[m, rows, :] = (r_v[m, rows, :].astype(F32) + g).astype(BF16)
        square[...] += jnp.sum((g * g).reshape(ROWS // 8, 8, width), 0)

    def send(item):
        chunk = lax.rem(item, chunks)
        m, rows = at(chunk)

        def copy(source, target):
            return pltpu.make_async_remote_copy(
                src_ref=source.at[m, rows],
                dst_ref=target.at[m, rows],
                send_sem=send_sem.at[item],
                recv_sem=recv_sem.at[item],
                device_id=(ahead,),
                device_id_type=pl.DeviceIdType.MESH,
            )

        return copy

    early, late = ((w_v, got_s), (mine, got_t)) if mutual else ((mine, got_t), (sent, got_s))

    def write_r(chunk):
        m, rows = at(chunk)
        return pltpu.make_async_copy(out_r.at[m, rows], new_r_hbm.at[m, rows], or_sem.at[chunk])

    def write_w(chunk):
        m, rows = at(chunk)
        return pltpu.make_async_copy(out_w.at[m, rows], new_w_hbm.at[m, rows], ow_sem.at[chunk])

    def on_tracked(chunk):
        m, rows = at(chunk)
        tracker = 0.5 * (mine[m, rows, :].astype(F32) + got_t[m, rows, :].astype(F32))
        w = w_v[m, rows, :].astype(F32)
        if mutual:
            theirs = (got_s[m, rows, :].astype(F32) - STEP_RATE * tracker).astype(BF16).astype(F32)
            out_w[m, rows, :] = (0.5 * w + 0.5 * theirs - 0.5 * STEP_RATE * tracker).astype(BF16)
        else:
            sent[m, rows, :] = (w - STEP_RATE * tracker).astype(BF16)
        out_r[m, rows, :] = (tracker - grad[m, rows, :]).astype(BF16)
        write_r(chunk).start()
        if mutual:
            write_w(chunk).start()

    def on_sent(chunk):
        m, rows = at(chunk)
        tracker = 0.5 * (mine[m, rows, :].astype(F32) + got_t[m, rows, :].astype(F32))
        w = w_v[m, rows, :].astype(F32)
        out_w[m, rows, :] = (0.5 * w + 0.5 * got_s[m, rows, :].astype(F32) - 0.5 * STEP_RATE * tracker).astype(BF16)
        write_w(chunk).start()

    def part_copy(k, d):
        start, size, place, others, places = groups[k]
        return pltpu.make_async_remote_copy(
            src_ref=parts.at[start + place],
            dst_ref=parts.at[start + place],
            send_sem=part_send.at[start + d],
            recv_sem=part_recv.at[start + place],
            device_id=(others[d],),
            device_id_type=pl.DeviceIdType.MESH,
        )

    def part_arrival(k, d):
        start, size, place, others, places = groups[k]
        return pltpu.make_async_remote_copy(
            src_ref=parts.at[start + places[d]],
            dst_ref=parts.at[start + places[d]],
            send_sem=part_send.at[start + d],
            recv_sem=part_recv.at[start + places[d]],
            device_id=(others[d],),
            device_id_type=pl.DeviceIdType.MESH,
        )

    def fold(k):
        start, size = groups[k][:2]
        value = parts[start]
        for n in range(1, size):
            value = value + parts[start + n]
        return value

    active = [k for k in range(len(groups)) if groups[k][1] > 1]

    def put_part(k, value):
        parts[groups[k][0] + groups[k][2]] = value

    def start_part(k):
        for d in range(groups[k][1] - 1):
            part_copy(k, d).start()

    def end_part(k):
        for d in range(groups[k][1] - 1):
            part_arrival(k, d).wait_recv()
        for d in range(groups[k][1] - 1):
            part_copy(k, d).wait_send()

    if mutual:
        for m in range(4):
            load_w(m).wait()
    else:
        compute(jnp.int32(0))
    pl.semaphore_wait(barrier, count)
    skip = 0 if mutual else 1
    first_part = chunks // 2 + 1

    def step(n, carry):
        @pl.when(n < 2 * chunks)
        def _():
            @pl.when(n >= WINDOW)
            def _():
                send(n - WINDOW)(*early).wait_send()

            @pl.when(n < chunks)
            def _():
                send(n)(*early).start()

            @pl.when(n >= chunks)
            def _():
                send(n)(*late).start()

        for extra in range(2):
            chunk = 2 * n + extra + skip

            @pl.when(chunk < chunks)
            def _():
                compute(chunk)

        for order, k in enumerate(active):

            @pl.when(n == first_part + 3 * order)
            def _():
                if order == 0:
                    value = square[:, :128]
                    for lanes in range(1, width // 128):
                        value = value + square[:, lanes * 128 : (lanes + 1) * 128]
                else:
                    end_part(active[order - 1])
                    value = fold(active[order - 1])
                put_part(k, value)

            @pl.when(n == first_part + 3 * order + 1)
            def _():
                start_part(k)

        got = n - WINDOW

        @pl.when(jnp.logical_and(got >= 0, got < chunks))
        def _():
            if not mutual:
                @pl.when(got == 0)
                def _():
                    for m in range(4):
                        load_w(m).wait()

            send(got)(*early).wait_recv()
            if not mutual:
                on_tracked(got)

        @pl.when(got >= chunks)
        def _():
            send(got)(*late).wait_recv()
            if mutual:
                on_tracked(got - chunks)
            else:
                on_sent(got - chunks)

        return carry

    lax.fori_loop(0, 2 * chunks + WINDOW, step, 0)
    end_part(active[-1])
    value = fold(active[-1])
    mean = jnp.sum(jnp.sum(value, 1, keepdims=True), 0, keepdims=True) / (total * 4 * width * width)
    rms_ref[0] = jnp.sqrt(jnp.broadcast_to(mean, (8, 128)))[0, 0]

    def drain(n, carry):
        write_r(n).wait()
        write_w(n).wait()
        return carry

    def settle(n, carry):
        send(n)(*late).wait_send()
        return carry

    lax.fori_loop(2 * chunks - WINDOW, 2 * chunks, settle, 0)
    lax.fori_loop(0, chunks, drain, 0)


def exchange_part(sizes, level, left, right, weights, residue):
    shape = weights.shape
    whole = (shape, BF16)
    chunks = 4 * (shape[-1] // ROWS)
    places = sum(sizes)
    dma = pltpu.SemaphoreType.DMA
    return pl.pallas_call(
        partial(exchange_kernel, sizes, 2**level),
        out_shape=(
            jax.ShapeDtypeStruct(shape, BF16),
            jax.ShapeDtypeStruct(shape, BF16),
            jax.ShapeDtypeStruct((1,), F32),
        ),
        in_specs=[pl.BlockSpec(memory_space=VMEM)] * 2 + [pl.BlockSpec(memory_space=ANY)] * 2,
        out_specs=(pl.BlockSpec(memory_space=ANY), pl.BlockSpec(memory_space=ANY), pl.BlockSpec(memory_space=SMEM)),
        scratch_shapes=[
            VMEM(*whole),
            VMEM(*whole),
            VMEM(shape, F32),
            VMEM(*whole),
            VMEM(*whole),
            VMEM(*whole),
            VMEM(*whole),
            VMEM(*whole),
            VMEM(*whole),
            VMEM((8, shape[-1]), F32),
            VMEM((places, 8, 128), F32),
            dma((4,)),
            dma((chunks,)),
            dma((2 * chunks,)),
            dma((2 * chunks,)),
            dma((chunks,)),
            dma((chunks,)),
            dma((places,)),
            dma((places,)),
        ],
        compiler_params=pltpu.CompilerParams(
            collective_id=level, has_side_effects=True, vmem_limit_bytes=40 << 20
        ),
        name=f"exchange_{level}",
    )(left, right, weights, residue)


def per_device(sizes, levels, round_index, sample_ids, token_pool, cotangent_pool, weights, residue):
    left, right = local_part(sample_ids, token_pool[0], cotangent_pool[0], weights[0])
    new_weights, new_residue, rms = lax.switch(
        round_index[0] % levels,
        [partial(exchange_part, sizes, level) for level in range(levels)],
        left,
        right,
        weights[0],
        residue[0],
    )
    return new_weights[None], new_residue[None], rms.reshape(())


def solution(mesh):
    nodes = mesh.shape["node"]
    sizes = {256: (8, 4, 4, 2), 16: (2, 2, 2, 2), 8: (2, 1, 2, 2), 4: (1, 1, 2, 2)}[nodes]
    levels = nodes.bit_length() - 1
    split = (P(), P("node", None)) + (P("node", None, None, None),) * 4
    return jax.shard_map(
        partial(per_device, sizes, levels),
        mesh=mesh,
        in_specs=split,
        out_specs=(P("node", None, None, None), P("node", None, None, None), P()),
        check_vma=False,
    )
```

```python
from functools import partial

import jax
import jax.numpy as jnp
from jax import lax
from jax.experimental import pallas as pl
from jax.experimental.pallas import tpu as pltpu
from jax.sharding import PartitionSpec as P

HEAD_DIM = 64
EPSILON = 1e-06
STEP_RATE = 0.1
ROWS = 128
WINDOW = 4
LAG = 4

F32, BF16 = jnp.float32, jnp.bfloat16
VMEM, SMEM, ANY = pltpu.VMEM, pltpu.SMEM, pl.ANY


def dot(a, b, contract):
    return lax.dot_general(a, b, ((contract[:1], contract[1:]), ((), ())), preferred_element_type=F32)


def local_kernel(ids_ref, token_ref, cot_ref, w_ref, left_ref, right_ref, q_s, k_s, v_s, c_s):
    pool, seq, width = token_ref.shape
    rows = pool * seq
    proj_scale = width**-0.5
    head_scale = HEAD_DIM**-0.5
    counts = []
    for image in range(pool):
        n = jnp.int32(0)
        for b in range(ids_ref.shape[1]):
            n = n + (ids_ref[0, b] == image).astype(jnp.int32)
        counts.append(n.astype(F32))

    x = token_ref[...].reshape(rows, width).astype(F32)
    centered = x - jnp.mean(x, -1, keepdims=True)
    variance = jnp.mean(centered * centered, -1, keepdims=True)
    normed = (centered * lax.rsqrt(variance + EPSILON)).astype(BF16)
    left_ref[0] = normed.T
    for which, out in enumerate((q_s, k_s, v_s)):
        out[...] = (dot(normed, w_ref[which], (1, 0)) * proj_scale).astype(BF16)
    cot = cot_ref[...].reshape(rows, width)
    right_ref[3] = cot
    cg = dot(cot, w_ref[3], (1, 1))
    for image in range(pool):
        at = slice(image * seq, (image + 1) * seq)
        c_s[at] = (cg[at] * (proj_scale * counts[image])).astype(BF16)

    pair = 2 * seq
    lane = lax.broadcasted_iota(jnp.int32, (pair, 128), 1) < HEAD_DIM
    near = lax.broadcasted_iota(jnp.int32, (seq, 128), 1) < seq
    zero = jnp.zeros((pair, 128), BF16)
    zero_half = jnp.zeros((seq, 128), BF16)

    def by_head(block):
        return jnp.concatenate([jnp.where(lane, block, zero), jnp.where(lane, zero, block)], 0)

    def packed(block):
        return jnp.where(near, block[:seq], block[seq:])

    def spread(block):
        return jnp.concatenate([jnp.where(near, block, zero_half), jnp.where(near, zero_half, block)], 0)

    for b in range(pool // 2):
        at = slice(b * pair, (b + 1) * pair)
        count = jnp.where(near[:1], counts[2 * b], counts[2 * b + 1])
        for j in range(width // 128):
            cols = slice(j * 128, (j + 1) * 128)
            q, k, v, c = q_s[at, cols], k_s[at, cols], v_s[at, cols], c_s[at, cols]
            kk, vv = by_head(k), by_head(v)
            scores = dot(kk, q, (1, 1)) * head_scale
            grads = dot(vv, c, (1, 1))
            probs, back = [], []
            for h in range(2):
                of_head = slice(h * pair, (h + 1) * pair)
                s = packed(scores[of_head])
                e = jnp.exp(s - jnp.max(s, 0, keepdims=True))
                p = e * (1.0 / jnp.sum(e, 0, keepdims=True))
                g = packed(grads[of_head])
                d = p * (g - jnp.sum(g * p, 0, keepdims=True)) * head_scale
                probs.append(spread(p.astype(BF16)))
                back.append(spread(d.astype(BF16)))
            p_rows, d_rows = jnp.concatenate(probs, 0), jnp.concatenate(back, 0)
            p_cols, d_cols = jnp.concatenate(probs, 1), jnp.concatenate(back, 1)
            left_ref[1, cols, at] = (dot(vv, p_rows, (0, 0)) * count).astype(BF16)
            right_ref[0, at, cols] = dot(d_rows, kk, (0, 0)).astype(BF16)
            right_ref[1, at, cols] = dot(d_cols, by_head(q), (1, 0)).astype(BF16)
            right_ref[2, at, cols] = dot(p_cols, by_head(c), (1, 0)).astype(BF16)


def local_part(sample_ids, tokens, cotangent, weights):
    pool, seq, width = tokens.shape
    rows = pool * seq
    return pl.pallas_call(
        local_kernel,
        out_shape=(
            jax.ShapeDtypeStruct((2, width, rows), BF16),
            jax.ShapeDtypeStruct((4, rows, width), BF16),
        ),
        in_specs=[pl.BlockSpec(memory_space=SMEM)] + [pl.BlockSpec(memory_space=VMEM)] * 3,
        out_specs=(pl.BlockSpec(memory_space=VMEM), pl.BlockSpec(memory_space=VMEM)),
        scratch_shapes=[VMEM((rows, width), BF16)] * 4,
        compiler_params=pltpu.CompilerParams(vmem_limit_bytes=32 << 20),
        cost_estimate=pl.CostEstimate(flops=2 * 4 * rows * width * width, bytes_accessed=4 << 20, transcendentals=rows * width),
        name="local",
    )(sample_ids, tokens, cotangent, weights)


def ring_leg(me, total, stride, size, carry):
    place = lax.rem(me // stride, size)
    down = lax.rem(me + jnp.where(place == 0, (size - 1) * stride, total - stride), total)
    up = lax.rem(me + jnp.where(place == size - 1, total - (size - 1) * stride, stride), total)
    if carry:
        down = jnp.where(place == size - 2, lax.rem(me + (size - 1) * stride, total), down)
        up = jnp.where(place == size - 3, lax.rem(me + total - (size - 1) * stride, total), up)
    return down, up


def jump_leg(me, total, jump):
    return lax.rem(me + jump, total), lax.rem(me + total - jump, total)


def detour(total, level):
    if total == 256:
        if level in (1, 3):
            return 4, [partial(ring_leg, total=total, stride=2**level, size=4, carry=leg == 1) for leg in range(3)]
        if level == 5:
            return 2, [partial(jump_leg, total=total, jump=jump) for jump in (160, 160, 224)]
        if level == 6:
            return 4, [partial(jump_leg, total=total, jump=jump) for jump in (160, 160)]
    if total == 8:
        if level == 0:
            return 4, [partial(ring_leg, total=total, stride=1, size=4, carry=leg == 1) for leg in range(3)]
        if level == 1:
            return 4, [partial(jump_leg, total=total, jump=jump) for jump in (5, 5)]
    return 0, []


def exchange_kernel(
    sizes,
    level,
    left_ref,
    right_ref,
    w_hbm,
    r_hbm,
    new_w_hbm,
    new_r_hbm,
    rms_ref,
    w_v,
    r_v,
    grad,
    mine,
    sent,
    got_t,
    got_s,
    out_w,
    out_r,
    square,
    parts,
    w_sem,
    r_sem,
    send_sem,
    recv_sem,
    ow_sem,
    or_sem,
    part_send,
    part_recv,
    relay=None,
    leg_send=None,
    leg_recv=None,
):
    distance = 2**level
    total = 1
    for size in sizes:
        total *= size
    width = w_hbm.shape[-1]
    per = width // ROWS
    chunks = 4 * per
    proj_scale = width**-0.5
    mutual = (2 * distance) % total == 0
    me = lax.axis_index("node")
    ahead = lax.rem(me + distance, total)
    behind = lax.rem(me + total - distance, total)
    away, legs = detour(total, level)
    paths = [leg(me) for leg in legs]
    near = chunks - away
    items = 2 * near
    hops = 2 * away * len(legs)

    groups = []
    stride = 1
    first = 0
    for size in reversed(sizes):
        place = lax.rem(me // stride, size)
        base = me - place * stride
        others = [base + lax.rem(place + d, size) * stride for d in range(1, size)]
        places = [lax.rem(place + d, size) for d in range(1, size)]
        groups.append((first, size, place, others, places))
        first += size
        stride *= size

    barrier = pltpu.get_barrier_semaphore()
    count = 1
    pl.semaphore_signal(barrier, inc=1, device_id=(behind,), device_id_type=pl.DeviceIdType.MESH)
    for _, source in paths:
        pl.semaphore_signal(barrier, inc=1, device_id=(source,), device_id_type=pl.DeviceIdType.MESH)
        count += 1
    for _, size, _, others, _ in groups:
        for other in others:
            pl.semaphore_signal(barrier, inc=1, device_id=(other,), device_id_type=pl.DeviceIdType.MESH)
            count += 1

    def at(chunk):
        return chunk // per, pl.ds(pl.multiple_of(lax.rem(chunk, per) * ROWS, ROWS), ROWS)

    def load_r(chunk):
        m, rows = at(chunk)
        return pltpu.make_async_copy(r_hbm.at[m, rows], r_v.at[m, rows], r_sem.at[chunk])

    def load_w(m):
        return pltpu.make_async_copy(w_hbm.at[m], w_v.at[m], w_sem.at[m])

    for chunk in range(chunks):
        load_r(jnp.int32(chunk)).start()
    for m in range(4):
        load_w(m).start()

    square[...] = jnp.zeros_like(square)

    def compute(chunk):
        m, rows = at(chunk)
        g = dot(left_ref[m // 3, rows, :], right_ref[m], (1, 0)) * proj_scale
        load_r(chunk).wait()
        grad[m, rows, :] = g
        mine[m, rows, :] = (r_v[m, rows, :].astype(F32) + g).astype(BF16)
        square[...] += jnp.sum((g * g).reshape(ROWS // 8, 8, width), 0)

    def send(item):
        m, rows = at(jnp.where(item < near, item, item - near + away))

        def copy(source, target):
            return pltpu.make_async_remote_copy(
                src_ref=source.at[m, rows],
                dst_ref=target.at[m, rows],
                send_sem=send_sem.at[item],
                recv_sem=recv_sem.at[item],
                device_id=(ahead,),
                device_id_type=pl.DeviceIdType.MESH,
            )

        return copy

    early, late = ((w_v, got_s), (mine, got_t)) if mutual else ((mine, got_t), (sent, got_s))

    def hop(phase, leg, j):
        m, rows = at((near + j, j)[phase])
        index = (phase * len(legs) + leg) * away + j
        mine_at, got_at = [((mine, got_t), (sent, got_s))[phase][k].at[m, rows] for k in range(2)]
        slot = [relay.at[(phase * (len(legs) - 1) + k) * away + j] for k in range(len(legs) - 1)]
        return pltpu.make_async_remote_copy(
            src_ref=mine_at if leg == 0 else slot[leg - 1],
            dst_ref=got_at if leg == len(legs) - 1 else slot[leg],
            send_sem=leg_send.at[index],
            recv_sem=leg_recv.at[index],
            device_id=(paths[leg][0],),
            device_id_type=pl.DeviceIdType.MESH,
        )

    def write_r(chunk):
        m, rows = at(chunk)
        return pltpu.make_async_copy(out_r.at[m, rows], new_r_hbm.at[m, rows], or_sem.at[chunk])

    def write_w(chunk):
        m, rows = at(chunk)
        return pltpu.make_async_copy(out_w.at[m, rows], new_w_hbm.at[m, rows], ow_sem.at[chunk])

    def on_tracked(chunk):
        m, rows = at(chunk)
        tracker = 0.5 * (mine[m, rows, :].astype(F32) + got_t[m, rows, :].astype(F32))
        w = w_v[m, rows, :].astype(F32)
        if mutual:
            theirs = (got_s[m, rows, :].astype(F32) - STEP_RATE * tracker).astype(BF16).astype(F32)
            out_w[m, rows, :] = (0.5 * w + 0.5 * theirs - 0.5 * STEP_RATE * tracker).astype(BF16)
        else:
            sent[m, rows, :] = (w - STEP_RATE * tracker).astype(BF16)
        out_r[m, rows, :] = (tracker - grad[m, rows, :]).astype(BF16)
        write_r(chunk).start()
        if mutual:
            write_w(chunk).start()

    def on_sent(chunk):
        m, rows = at(chunk)
        tracker = 0.5 * (mine[m, rows, :].astype(F32) + got_t[m, rows, :].astype(F32))
        w = w_v[m, rows, :].astype(F32)
        out_w[m, rows, :] = (0.5 * w + 0.5 * got_s[m, rows, :].astype(F32) - 0.5 * STEP_RATE * tracker).astype(BF16)
        write_w(chunk).start()

    def part_copy(k, d):
        start, size, place, others, places = groups[k]
        return pltpu.make_async_remote_copy(
            src_ref=parts.at[start + place],
            dst_ref=parts.at[start + place],
            send_sem=part_send.at[start + d],
            recv_sem=part_recv.at[start + place],
            device_id=(others[d],),
            device_id_type=pl.DeviceIdType.MESH,
        )

    def part_arrival(k, d):
        start, size, place, others, places = groups[k]
        return pltpu.make_async_remote_copy(
            src_ref=parts.at[start + places[d]],
            dst_ref=parts.at[start + places[d]],
            send_sem=part_send.at[start + d],
            recv_sem=part_recv.at[start + places[d]],
            device_id=(others[d],),
            device_id_type=pl.DeviceIdType.MESH,
        )

    def fold(k):
        start, size = groups[k][:2]
        value = parts[start]
        for n in range(1, size):
            value = value + parts[start + n]
        return value

    active = [k for k in range(len(groups)) if groups[k][1] > 1]

    def put_part(k, value):
        parts[groups[k][0] + groups[k][2]] = value

    def start_part(k):
        for d in range(groups[k][1] - 1):
            part_copy(k, d).start()

    def end_part(k):
        for d in range(groups[k][1] - 1):
            part_arrival(k, d).wait_recv()
        for d in range(groups[k][1] - 1):
            part_copy(k, d).wait_send()

    def order(k):
        if not away:
            return k
        early_k = jnp.where(lax.rem(k, 2) == 0, k // 2, near + k // 2)
        return jnp.where(k < 2 * away, early_k, k - away)

    if mutual:
        for m in range(4):
            load_w(m).wait()
    else:
        compute(jnp.int32(0))
    pl.semaphore_wait(barrier, count)
    skip = 0 if mutual else 1
    first_part = chunks // 2 + 1

    def hops_at(n, act):
        low, high = (n * hops) // items, ((n + 1) * hops) // items
        for phase in range(2):
            for leg in range(len(legs)):
                start = (phase * len(legs) + leg) * away

                @pl.when(jnp.logical_and(jnp.logical_and(n >= 0, high > low), jnp.logical_and(low >= start, low < start + away)))
                def _(phase=phase, leg=leg, start=start):
                    act(phase, leg, low - start)

    def start_hop(phase, leg, j):
        if leg:
            hop(phase, leg - 1, j).wait_recv()
        hop(phase, leg, j).start()

    def end_hop(phase, leg, j):
        if leg == len(legs) - 1:
            hop(phase, leg, j).wait_recv()
            if phase == 0:
                on_tracked(near + j)
            else:
                on_sent(j)

    def step(n, carry):
        @pl.when(n < items)
        def _():
            @pl.when(n >= WINDOW)
            def _():
                send(n - WINDOW)(*early).wait_send()

            @pl.when(n < near)
            def _():
                send(n)(*early).start()

            @pl.when(n >= near)
            def _():
                send(n)(*late).start()

        if away:
            hops_at(n - 1, start_hop)

        for extra in range(2):
            chunk = 2 * n + extra + skip

            @pl.when(chunk < chunks)
            def _():
                compute(order(chunk))

        for turn, k in enumerate(active):

            @pl.when(n == first_part + 3 * turn)
            def _():
                if turn == 0:
                    value = square[:, :128]
                    for lanes in range(1, width // 128):
                        value = value + square[:, lanes * 128 : (lanes + 1) * 128]
                else:
                    end_part(active[turn - 1])
                    value = fold(active[turn - 1])
                put_part(k, value)

            @pl.when(n == first_part + 3 * turn + 1)
            def _():
                start_part(k)

        got = n - WINDOW

        @pl.when(jnp.logical_and(got >= 0, got < near))
        def _():
            if not mutual:
                @pl.when(got == 0)
                def _():
                    for m in range(4):
                        load_w(m).wait()

            send(got)(*early).wait_recv()
            if not mutual:
                on_tracked(got)

        @pl.when(jnp.logical_and(got >= near, got < items))
        def _():
            send(got)(*late).wait_recv()
            if mutual:
                on_tracked(got - near)
            else:
                on_sent(got - near + away)

        if away:
            hops_at(n - 1 - LAG, end_hop)

        return carry

    lax.fori_loop(0, items + max(WINDOW, LAG + 1 if away else 0), step, 0)
    end_part(active[-1])
    value = fold(active[-1])
    mean = jnp.sum(jnp.sum(value, 1, keepdims=True), 0, keepdims=True) / (total * 4 * width * width)
    rms_ref[0] = jnp.sqrt(jnp.broadcast_to(mean, (8, 128)))[0, 0]

    def drain(n, carry):
        write_r(n).wait()
        write_w(n).wait()
        return carry

    def settle(n, carry):
        send(n)(*late).wait_send()
        return carry

    lax.fori_loop(items - WINDOW, items, settle, 0)
    for phase in range(2):
        for leg in range(len(legs)):

            def settle_hop(j, carry, phase=phase, leg=leg):
                hop(phase, leg, j).wait_send()
                return carry

            lax.fori_loop(0, away, settle_hop, 0)
    lax.fori_loop(0, chunks, drain, 0)


def len_bits(sizes):
    return sum(size.bit_length() - 1 for size in sizes)


def exchange_part(sizes, level, left, right, weights, residue):
    shape = weights.shape
    whole = (shape, BF16)
    chunks = 4 * (shape[-1] // ROWS)
    places = sum(sizes)
    away, legs = detour(2 ** len_bits(sizes), level)
    dma = pltpu.SemaphoreType.DMA
    return pl.pallas_call(
        partial(exchange_kernel, sizes, level),
        out_shape=(
            jax.ShapeDtypeStruct(shape, BF16),
            jax.ShapeDtypeStruct(shape, BF16),
            jax.ShapeDtypeStruct((1,), F32),
        ),
        in_specs=[pl.BlockSpec(memory_space=VMEM)] * 2 + [pl.BlockSpec(memory_space=ANY)] * 2,
        out_specs=(pl.BlockSpec(memory_space=ANY), pl.BlockSpec(memory_space=ANY), pl.BlockSpec(memory_space=SMEM)),
        scratch_shapes=[
            VMEM(*whole),
            VMEM(*whole),
            VMEM(shape, F32),
            VMEM(*whole),
            VMEM(*whole),
            VMEM(*whole),
            VMEM(*whole),
            VMEM(*whole),
            VMEM(*whole),
            VMEM((8, shape[-1]), F32),
            VMEM((places, 8, 128), F32),
            dma((4,)),
            dma((chunks,)),
            dma((2 * chunks,)),
            dma((2 * chunks,)),
            dma((chunks,)),
            dma((chunks,)),
            dma((places,)),
            dma((places,)),
        ]
        + (
            [
                VMEM((2 * (len(legs) - 1) * away, ROWS, shape[-1]), BF16),
                dma((2 * len(legs) * away,)),
                dma((2 * len(legs) * away,)),
            ]
            if away
            else []
        ),
        compiler_params=pltpu.CompilerParams(
            collective_id=level, has_side_effects=True, vmem_limit_bytes=40 << 20
        ),
        name=f"exchange_{level}",
    )(left, right, weights, residue)


def per_device(sizes, levels, round_index, sample_ids, token_pool, cotangent_pool, weights, residue):
    left, right = local_part(sample_ids, token_pool[0], cotangent_pool[0], weights[0])
    new_weights, new_residue, rms = lax.switch(
        round_index[0] % levels,
        [partial(exchange_part, sizes, level) for level in range(levels)],
        left,
        right,
        weights[0],
        residue[0],
    )
    return new_weights[None], new_residue[None], rms.reshape(())


def solution(mesh):
    nodes = mesh.shape["node"]
    sizes = {256: (8, 4, 4, 2), 16: (2, 2, 2, 2), 8: (2, 1, 4, 1), 4: (1, 1, 2, 2)}[nodes]
    levels = nodes.bit_length() - 1
    split = (P(), P("node", None)) + (P("node", None, None, None),) * 4
    return jax.shard_map(
        partial(per_device, sizes, levels),
        mesh=mesh,
        in_specs=split,
        out_specs=(P("node", None, None, None), P("node", None, None, None), P()),
        check_vma=False,
    )
```

```python
from functools import partial

import jax
import jax.numpy as jnp
from jax import lax
from jax.experimental import pallas as pl
from jax.experimental.pallas import tpu as pltpu
from jax.sharding import PartitionSpec as P

HEAD_DIM = 64
EPSILON = 1e-06
STEP_RATE = 0.1
ROWS = 128
WINDOW = 6
LAG = 4
LEAD = 2
RELAYS = 8
BURST = 4

F32, BF16 = jnp.float32, jnp.bfloat16
VMEM, SMEM, ANY = pltpu.VMEM, pltpu.SMEM, pl.ANY


def dot(a, b, contract):
    return lax.dot_general(a, b, ((contract[:1], contract[1:]), ((), ())), preferred_element_type=F32)


def local_kernel(
    ids_hbm, token_hbm, cot_hbm, w_hbm, left_ref, right_ref, ids_ref, token_ref, w_ref, q_s, k_s, v_s, c_s, sems
):
    pool, seq, width = token_hbm.shape
    rows = pool * seq
    proj_scale = width**-0.5
    head_scale = HEAD_DIM**-0.5
    loads = [
        pltpu.make_async_copy(ids_hbm, ids_ref, sems.at[0]),
        pltpu.make_async_copy(token_hbm, token_ref, sems.at[1]),
    ]
    loads += [pltpu.make_async_copy(w_hbm.at[m], w_ref.at[m], sems.at[2 + m]) for m in range(4)]
    loads += [
        pltpu.make_async_copy(cot_hbm.at[image], right_ref.at[3, pl.ds(image * seq, seq)], sems.at[6 + image])
        for image in range(pool)
    ]
    for load in loads:
        load.start()
    loads[0].wait()
    counts = []
    for image in range(pool):
        n = jnp.int32(0)
        for b in range(ids_ref.shape[1]):
            n = n + (ids_ref[0, b] == image).astype(jnp.int32)
        counts.append(n.astype(F32))

    loads[1].wait()
    x = token_ref[...].reshape(rows, width).astype(F32)
    centered = x - jnp.mean(x, -1, keepdims=True)
    variance = jnp.mean(centered * centered, -1, keepdims=True)
    normed = (centered * lax.rsqrt(variance + EPSILON)).astype(BF16)
    left_ref[0] = normed.T
    for which, out in enumerate((q_s, k_s, v_s)):
        loads[2 + which].wait()
        out[...] = (dot(normed, w_ref[which], (1, 0)) * proj_scale).astype(BF16)
    loads[5].wait()
    for load in loads[6:]:
        load.wait()
    cg = dot(right_ref[3], w_ref[3], (1, 1))
    for image in range(pool):
        at = slice(image * seq, (image + 1) * seq)
        c_s[at] = (cg[at] * (proj_scale * counts[image])).astype(BF16)

    pair = 2 * seq
    lane = lax.broadcasted_iota(jnp.int32, (pair, 128), 1) < HEAD_DIM
    near = lax.broadcasted_iota(jnp.int32, (seq, 128), 1) < seq
    zero = jnp.zeros((pair, 128), BF16)
    zero_half = jnp.zeros((seq, 128), BF16)

    def by_head(block):
        return jnp.concatenate([jnp.where(lane, block, zero), jnp.where(lane, zero, block)], 0)

    def packed(block):
        return jnp.where(near, block[:seq], block[seq:])

    def spread(block):
        return jnp.concatenate([jnp.where(near, block, zero_half), jnp.where(near, zero_half, block)], 0)

    blocks = []
    for b in range(pool // 2):
        for j in range(width // 128):
            blocks.append((slice(b * pair, (b + 1) * pair), slice(j * 128, (j + 1) * 128)))
    group = 4
    for first in range(0, len(blocks), group):
        some = blocks[first : first + group]
        score = [dot(by_head(k_s[at, cols]), q_s[at, cols], (1, 1)) * head_scale for at, cols in some]
        grads = [dot(by_head(v_s[at, cols]), c_s[at, cols], (1, 1)) for at, cols in some]
        probs, back = [], []
        for block in range(len(some)):
            probs.append([])
            back.append([])
            for h in range(2):
                of_head = slice(h * pair, (h + 1) * pair)
                s = packed(score[block][of_head])
                e = jnp.exp(s - jnp.max(s, 0, keepdims=True))
                p = e * (1.0 / jnp.sum(e, 0, keepdims=True))
                g = packed(grads[block][of_head])
                d = p * (g - jnp.sum(g * p, 0, keepdims=True)) * head_scale
                probs[-1].append(spread(p.astype(BF16)))
                back[-1].append(spread(d.astype(BF16)))
        for block, (at, cols) in enumerate(some):
            b = at.start // pair
            count = jnp.where(near[:1], counts[2 * b], counts[2 * b + 1])
            context = dot(by_head(v_s[at, cols]), jnp.concatenate(probs[block], 0), (0, 0))
            left_ref[1, cols, at] = (context * count).astype(BF16)
            right_ref[0, at, cols] = dot(jnp.concatenate(back[block], 0), by_head(k_s[at, cols]), (0, 0)).astype(BF16)
            right_ref[1, at, cols] = dot(jnp.concatenate(back[block], 1), by_head(q_s[at, cols]), (1, 0)).astype(BF16)
            right_ref[2, at, cols] = dot(jnp.concatenate(probs[block], 1), by_head(c_s[at, cols]), (1, 0)).astype(BF16)


def local_part(sample_ids, tokens, cotangent, weights):
    pool, seq, width = tokens.shape
    rows = pool * seq
    return pl.pallas_call(
        local_kernel,
        out_shape=(
            jax.ShapeDtypeStruct((2, width, rows), BF16),
            jax.ShapeDtypeStruct((4, rows, width), BF16),
        ),
        in_specs=[pl.BlockSpec(memory_space=ANY)] * 4,
        out_specs=(pl.BlockSpec(memory_space=VMEM), pl.BlockSpec(memory_space=VMEM)),
        scratch_shapes=[
            SMEM(sample_ids.shape, jnp.int32),
            VMEM(tokens.shape, BF16),
            VMEM(weights.shape, BF16),
        ]
        + [VMEM((rows, width), BF16)] * 4
        + [pltpu.SemaphoreType.DMA((6 + pool,))],
        compiler_params=pltpu.CompilerParams(vmem_limit_bytes=32 << 20),
        cost_estimate=pl.CostEstimate(flops=2 * 4 * rows * width * width, bytes_accessed=4 << 20, transcendentals=rows * width),
        name="local",
    )(*[pltpu.with_memory_space_constraint(x, pltpu.HBM) for x in (sample_ids, tokens, cotangent, weights)])


def ring_leg(me, total, stride, size, carry):
    place = lax.rem(me // stride, size)
    down = lax.rem(me + jnp.where(place == 0, (size - 1) * stride, total - stride), total)
    up = lax.rem(me + jnp.where(place == size - 1, total - (size - 1) * stride, stride), total)
    if carry:
        down = jnp.where(place == size - 2, lax.rem(me + (size - 1) * stride, total), down)
        up = jnp.where(place == size - 3, lax.rem(me + total - (size - 1) * stride, total), up)
    return down, up


def jump_leg(me, total, jump):
    return lax.rem(me + jump, total), lax.rem(me + total - jump, total)


def snake_place(z):
    return jnp.where(lax.rem(z, 2) == 1, (z + 1) // 2, lax.rem(8 - z // 2, 8))


def snake_at(place):
    return jnp.where(place == 0, 0, jnp.where(place < 5, 2 * place - 1, 16 - 2 * place))


def detour(total, level):
    if total == 256:
        if level in (1, 3):
            return 4, [partial(ring_leg, total=total, stride=2**level, size=4, carry=leg == 1) for leg in range(3)]
        if level == 5:
            return 2, [partial(jump_leg, total=total, jump=jump) for jump in (160, 160, 224)]
        if level == 6:
            return 4, [partial(jump_leg, total=total, jump=jump) for jump in (160, 160)]
    if total == 8:
        if level == 0:
            return 4, [partial(ring_leg, total=total, stride=1, size=4, carry=leg == 1) for leg in range(3)]
        if level == 1:
            return 4, [partial(jump_leg, total=total, jump=jump) for jump in (5, 5)]
    return 0, []


def exchange_kernel(
    sizes,
    level,
    left_ref,
    right_ref,
    w_hbm,
    r_hbm,
    new_w_hbm,
    new_r_hbm,
    rms_ref,
    w_v,
    r_v,
    grad,
    mine,
    sent,
    got_t,
    got_s,
    out_w,
    out_r,
    square,
    parts,
    w_sem,
    r_sem,
    send_sem,
    recv_sem,
    ow_sem,
    or_sem,
    part_send,
    part_recv,
    rms_s,
    rms_sem,
    relay=None,
    leg_send=None,
    leg_recv=None,
):
    distance = 2**level
    total = 1
    for size in sizes:
        total *= size
    width = w_hbm.shape[-1]
    per = width // ROWS
    chunks = 4 * per
    proj_scale = width**-0.5
    mutual = (2 * distance) % total == 0
    me = lax.axis_index("node")
    ahead = lax.rem(me + distance, total)
    behind = lax.rem(me + total - distance, total)
    away, legs = detour(total, level)
    paths = [leg(me) for leg in legs]
    near = chunks - away
    items = 2 * near
    hops = 2 * away * len(legs)

    groups = []
    strides = []
    stride = 1
    first = 0
    for size in reversed(sizes):
        place = lax.rem(me // stride, size)
        base = me - place * stride
        snake = size == 8 and distance < stride
        if snake:
            place = snake_place(place)
            others = [base + snake_at(lax.rem(place + d, size)) * stride for d in (1, size - 1)]
        else:
            others = [base + lax.rem(place + d, size) * stride for d in range(1, size)]
        places = [lax.rem(place + d, size) for d in range(1, size)]
        groups.append((first, size, place, others, places, snake))
        strides.append(stride)
        first += size
        stride *= size

    barrier = pltpu.get_barrier_semaphore()
    count = 1
    pl.semaphore_signal(barrier, inc=1, device_id=(behind,), device_id_type=pl.DeviceIdType.MESH)
    for _, source in paths:
        pl.semaphore_signal(barrier, inc=1, device_id=(source,), device_id_type=pl.DeviceIdType.MESH)
        count += 1
    for _, _, _, others, _, _ in groups:
        for other in others:
            pl.semaphore_signal(barrier, inc=1, device_id=(other,), device_id_type=pl.DeviceIdType.MESH)
            count += 1

    def at(chunk):
        return chunk // per, pl.ds(pl.multiple_of(lax.rem(chunk, per) * ROWS, ROWS), ROWS)

    def load_r(m):
        return pltpu.make_async_copy(r_hbm.at[m], r_v.at[m], r_sem.at[m])

    load_w = pltpu.make_async_copy(w_hbm, w_v, w_sem)

    for m in range(4):
        load_r(m).start()
    load_w.start()

    square[...] = jnp.zeros_like(square)

    def compute(chunk):
        m, rows = at(chunk)
        g = dot(left_ref[m // 3, rows, :], right_ref[m], (1, 0)) * proj_scale
        grad[m, rows, :] = g
        mine[m, rows, :] = (r_v[m, rows, :].astype(F32) + g).astype(BF16)
        square[...] += jnp.sum((g * g).reshape(ROWS // 8, 8, width), 0)

    def send(item):
        m, rows = at(jnp.where(item < near, item, item - near + away))

        def copy(source, target):
            return pltpu.make_async_remote_copy(
                src_ref=source.at[m, rows],
                dst_ref=target.at[m, rows],
                send_sem=send_sem.at[lax.rem(item, WINDOW)],
                recv_sem=recv_sem.at[item],
                device_id=(ahead,),
                device_id_type=pl.DeviceIdType.MESH,
            )

        return copy

    early, late = ((w_v, got_s), (mine, got_t)) if mutual else ((mine, got_t), (sent, got_s))

    def hop(phase, leg, j):
        m, rows = at((near + j, j)[phase])
        index = (phase * len(legs) + leg) * away + j
        mine_at, got_at = [((mine, got_t), (sent, got_s))[phase][k].at[m, rows] for k in range(2)]
        slot = [relay.at[(phase * (len(legs) - 1) + k) * away + j] for k in range(len(legs) - 1)]
        return pltpu.make_async_remote_copy(
            src_ref=mine_at if leg == 0 else slot[leg - 1],
            dst_ref=got_at if leg == len(legs) - 1 else slot[leg],
            send_sem=leg_send.at[lax.rem(index, RELAYS)],
            recv_sem=leg_recv.at[index],
            device_id=(paths[leg][0],),
            device_id_type=pl.DeviceIdType.MESH,
        )

    def write_r(chunk):
        m, rows = at(chunk)
        return pltpu.make_async_copy(out_r.at[m, rows], new_r_hbm.at[m, rows], or_sem)

    def write_w(chunk):
        m, rows = at(chunk)
        return pltpu.make_async_copy(out_w.at[m, rows], new_w_hbm.at[m, rows], ow_sem)

    def on_tracked(chunk):
        m, rows = at(chunk)
        tracker = 0.5 * (mine[m, rows, :].astype(F32) + got_t[m, rows, :].astype(F32))
        w = w_v[m, rows, :].astype(F32)
        if mutual:
            theirs = (got_s[m, rows, :].astype(F32) - STEP_RATE * tracker).astype(BF16).astype(F32)
            out_w[m, rows, :] = (0.5 * w + 0.5 * theirs - 0.5 * STEP_RATE * tracker).astype(BF16)
        else:
            sent[m, rows, :] = (w - STEP_RATE * tracker).astype(BF16)
        out_r[m, rows, :] = (tracker - grad[m, rows, :]).astype(BF16)
        write_r(chunk).start()
        if mutual:
            write_w(chunk).start()

    def on_sent(chunk):
        m, rows = at(chunk)
        tracker = 0.5 * (mine[m, rows, :].astype(F32) + got_t[m, rows, :].astype(F32))
        w = w_v[m, rows, :].astype(F32)
        out_w[m, rows, :] = (0.5 * w + 0.5 * got_s[m, rows, :].astype(F32) - 0.5 * STEP_RATE * tracker).astype(BF16)
        write_w(chunk).start()

    def part_copy(device, slot, sem):
        return pltpu.make_async_remote_copy(
            src_ref=parts.at[slot],
            dst_ref=parts.at[slot],
            send_sem=part_send.at[sem],
            recv_sem=part_recv.at[slot],
            device_id=(device,),
            device_id_type=pl.DeviceIdType.MESH,
        )

    def part_moves(k, turn):
        start, size, place, others, places, snake = groups[k]
        if not snake:
            return [(others[d], start + place, d) for d in range(size - 1)], [start + p for p in places]
        held = [start + lax.rem(place + d, size) for d in range(size)]
        sends = [(others[0], held[-turn % size], 0)]
        arrivals = [held[-turn - 1]]
        if turn < (size - 1) // 2:
            sends.append((others[-1], held[turn], 1))
            arrivals.append(held[turn + 1])
        return sends, arrivals

    def loaded(k):
        return strides[k] <= distance < strides[k] * groups[k][1]

    turns = []
    tick = -(-(chunks - 1) // BURST) + 1
    last = max(k for k in range(len(groups)) if loaded(k) or (distance == 1 and k == 1))
    for k in [k for k in range(len(groups)) if k != last] + [last]:
        if groups[k][1] > 1:
            for turn in range(groups[k][1] // 2 if groups[k][5] else 1):
                turns.append((tick, k, turn))
                tick += 4 if distance == 1 else 2
    last_tick = max(tick, items + max(WINDOW, LAG + 1 if away else 0))

    def fold(k):
        start, size = groups[k][:2]
        value = parts[start]
        for n in range(1, size):
            value = value + parts[start + n]
        return value

    def end_part(k, turn):
        sends, arrivals = part_moves(k, turn)
        for slot in arrivals:
            part_copy(me, slot, 0).wait_recv()
        for device, slot, sem in sends:
            part_copy(device, slot, sem).wait_send()

    def next_part(index):
        if index:
            end_part(*turns[index - 1][1:])
        if index == len(turns):
            value = fold(turns[-1][1])
            mean = jnp.sum(jnp.sum(value, 1, keepdims=True), 0, keepdims=True) / (total * 4 * width * width)
            rms_s[0] = jnp.sqrt(jnp.broadcast_to(mean, (8, 128)))[0, 0]
            rms_copy().start()
        elif turns[index][2] == 0:
            if index:
                value = fold(turns[index - 1][1])
            else:
                value = square[:, :128]
                for lanes in range(1, width // 128):
                    value = value + square[:, lanes * 128 : (lanes + 1) * 128]
            k = turns[index][1]
            parts[groups[k][0] + groups[k][2]] = value

    def start_part(index):
        for device, slot, sem in part_moves(*turns[index][1:])[0]:
            part_copy(device, slot, sem).start()

    def rms_copy():
        return pltpu.make_async_copy(rms_s, rms_ref, rms_sem)

    def order(k):
        if not away:
            return k
        early_k = jnp.where(lax.rem(k, 2) == 0, k // 2, near + k // 2)
        return jnp.where(k < 2 * away, early_k, k - away)

    if mutual:
        load_w.wait()
    load_r(0).wait()
    if not mutual:
        compute(jnp.int32(0))
    pl.semaphore_wait(barrier, count)
    for m in range(1, 4):
        load_r(m).wait()
    skip = 0 if mutual else 1

    def begun(n):
        return jnp.where(n <= 0, 0, jnp.minimum(hops, (n * hops) // items + jnp.minimum(n, LEAD)))

    def hops_at(n, act):
        def one(index, carry):
            for phase in range(2):
                for leg in range(len(legs)):
                    start = (phase * len(legs) + leg) * away

                    @pl.when(jnp.logical_and(index >= start, index < start + away))
                    def _(phase=phase, leg=leg, start=start):
                        act(phase, leg, index - start)

            return carry

        lax.fori_loop(begun(n), begun(n + 1), one, 0)

    def start_hop(phase, leg, j):
        @pl.when((phase * len(legs) + leg) * away + j >= RELAYS)
        def _():
            hop(phase, leg, j).wait_send()

        if leg:
            hop(phase, leg - 1, j).wait_recv()
        hop(phase, leg, j).start()

    def end_hop(phase, leg, j):
        if leg == len(legs) - 1:
            hop(phase, leg, j).wait_recv()
            if phase == 0:
                on_tracked(near + j)
            else:
                on_sent(j)

    def step(n, carry):
        @pl.when(n < items)
        def _():
            @pl.when(n >= WINDOW)
            def _():
                send(n - WINDOW)(*early).wait_send()

            @pl.when(n < near)
            def _():
                send(n)(*early).start()

            @pl.when(n >= near)
            def _():
                send(n)(*late).start()

        if away:
            hops_at(n - 1, start_hop)

        @pl.when(n <= chunks // BURST)
        def _():
            def some(k, carry):
                compute(order(k))
                return carry

            lax.fori_loop(n * BURST + skip, jnp.minimum((n + 1) * BURST + skip, chunks), some, 0)

        for index, (tick, _, _) in enumerate(turns):

            @pl.when(n == tick)
            def _(index=index):
                next_part(index)

        got = n - WINDOW

        @pl.when(jnp.logical_and(got >= 0, got < near))
        def _():
            if not mutual:
                @pl.when(got == 0)
                def _():
                    load_w.wait()

            send(got)(*early).wait_recv()
            if not mutual:
                on_tracked(got)

        @pl.when(jnp.logical_and(got >= near, got < items))
        def _():
            send(got)(*late).wait_recv()
            if mutual:
                on_tracked(got - near)
            else:
                on_sent(got - near + away)

        if away:
            hops_at(n - 1 - LAG, end_hop)

        for index, (tick, _, _) in enumerate(turns):

            @pl.when(n == tick)
            def _(index=index):
                start_part(index)

        return carry

    lax.fori_loop(0, last_tick, step, 0)
    next_part(len(turns))
    def settle(n, carry):
        send(n)(*late).wait_send()
        return carry

    lax.fori_loop(items - WINDOW, items, settle, 0)
    for index in range(max(0, hops - RELAYS), hops):
        hop(index // (len(legs) * away), index // away % len(legs), index % away).wait_send()
    pltpu.make_async_copy(out_r, new_r_hbm, or_sem).wait()
    pltpu.make_async_copy(out_w, new_w_hbm, ow_sem).wait()
    rms_copy().wait()


def len_bits(sizes):
    return sum(size.bit_length() - 1 for size in sizes)


def exchange_part(sizes, level, left, right, weights, residue):
    shape = weights.shape
    whole = (shape, BF16)
    chunks = 4 * (shape[-1] // ROWS)
    places = sum(sizes)
    away, legs = detour(2 ** len_bits(sizes), level)
    dma = pltpu.SemaphoreType.DMA
    return pl.pallas_call(
        partial(exchange_kernel, sizes, level),
        out_shape=(
            jax.ShapeDtypeStruct(shape, BF16),
            jax.ShapeDtypeStruct(shape, BF16),
            jax.ShapeDtypeStruct((1,), F32),
        ),
        in_specs=[pl.BlockSpec(memory_space=VMEM)] * 2 + [pl.BlockSpec(memory_space=ANY)] * 2,
        out_specs=(pl.BlockSpec(memory_space=ANY),) * 3,
        scratch_shapes=[
            VMEM(*whole),
            VMEM(*whole),
            VMEM(shape, F32),
            VMEM(*whole),
            VMEM(*whole),
            VMEM(*whole),
            VMEM(*whole),
            VMEM(*whole),
            VMEM(*whole),
            VMEM((8, shape[-1]), F32),
            VMEM((places, 8, 128), F32),
            dma,
            dma((4,)),
            dma((WINDOW,)),
            dma((2 * chunks,)),
            dma,
            dma,
            dma((max(sizes),)),
            dma((places,)),
            SMEM((1,), F32),
            dma,
        ]
        + (
            [
                VMEM((2 * (len(legs) - 1) * away, ROWS, shape[-1]), BF16),
                dma((RELAYS,)),
                dma((2 * len(legs) * away,)),
            ]
            if away
            else []
        ),
        compiler_params=pltpu.CompilerParams(
            collective_id=level, has_side_effects=True, vmem_limit_bytes=40 << 20
        ),
        name=f"exchange_{level}",
    )(left, right, weights, residue)


def per_device(sizes, levels, round_index, sample_ids, token_pool, cotangent_pool, weights, residue):
    left, right = local_part(sample_ids, token_pool[0], cotangent_pool[0], weights[0])
    new_weights, new_residue, rms = lax.switch(
        round_index[0] % levels,
        [partial(exchange_part, sizes, level) for level in range(levels)],
        left,
        right,
        weights[0],
        residue[0],
    )
    return new_weights[None], new_residue[None], rms.reshape(())


def solution(mesh):
    nodes = mesh.shape["node"]
    sizes = {256: (8, 4, 4, 2), 16: (2, 2, 2, 2), 8: (2, 1, 4, 1), 4: (1, 1, 2, 2)}[nodes]
    levels = nodes.bit_length() - 1
    split = (P(), P("node", None)) + (P("node", None, None, None),) * 4
    return jax.shard_map(
        partial(per_device, sizes, levels),
        mesh=mesh,
        in_specs=split,
        out_specs=(P("node", None, None, None), P("node", None, None, None), P()),
        check_vma=False,
    )
```

```python
from functools import partial

import jax
import jax.numpy as jnp
from jax import lax
from jax.experimental import pallas as pl
from jax.experimental.pallas import tpu as pltpu
from jax.sharding import PartitionSpec as P

HEAD_DIM = 64
EPSILON = 1e-06
STEP_RATE = 0.1
ROWS = 128
WINDOW = 6
LAG = 4
LEAD = 0
RELAYS = 8
BURST = 4

F32, BF16 = jnp.float32, jnp.bfloat16
VMEM, SMEM, ANY = pltpu.VMEM, pltpu.SMEM, pl.ANY


def dot(a, b, contract):
    return lax.dot_general(a, b, ((contract[:1], contract[1:]), ((), ())), preferred_element_type=F32)


def local_kernel(
    ids_hbm, token_hbm, cot_hbm, w_hbm, left_ref, right_ref, ids_ref, token_ref, w_ref, q_s, k_s, v_s, c_s, sems
):
    pool, seq, width = token_hbm.shape
    rows = pool * seq
    proj_scale = width**-0.5
    head_scale = HEAD_DIM**-0.5
    loads = [
        pltpu.make_async_copy(ids_hbm, ids_ref, sems.at[0]),
        pltpu.make_async_copy(token_hbm, token_ref, sems.at[1]),
    ]
    loads += [pltpu.make_async_copy(w_hbm.at[m], w_ref.at[m], sems.at[2 + m]) for m in range(4)]
    loads += [
        pltpu.make_async_copy(cot_hbm.at[image], right_ref.at[3, pl.ds(image * seq, seq)], sems.at[6 + image])
        for image in range(pool)
    ]
    for load in loads:
        load.start()
    loads[0].wait()
    counts = []
    for image in range(pool):
        n = jnp.int32(0)
        for b in range(ids_ref.shape[1]):
            n = n + (ids_ref[0, b] == image).astype(jnp.int32)
        counts.append(n.astype(F32))

    loads[1].wait()
    x = token_ref[...].reshape(rows, width).astype(F32)
    centered = x - jnp.mean(x, -1, keepdims=True)
    variance = jnp.mean(centered * centered, -1, keepdims=True)
    normed = (centered * lax.rsqrt(variance + EPSILON)).astype(BF16)
    left_ref[0] = normed.T
    for which, out in enumerate((q_s, k_s, v_s)):
        loads[2 + which].wait()
        out[...] = (dot(normed, w_ref[which], (1, 0)) * proj_scale).astype(BF16)
    loads[5].wait()
    for load in loads[6:]:
        load.wait()
    cg = dot(right_ref[3], w_ref[3], (1, 1))
    for image in range(pool):
        at = slice(image * seq, (image + 1) * seq)
        c_s[at] = (cg[at] * (proj_scale * counts[image])).astype(BF16)

    pair = 2 * seq
    lane = lax.broadcasted_iota(jnp.int32, (pair, 128), 1) < HEAD_DIM
    near = lax.broadcasted_iota(jnp.int32, (seq, 128), 1) < seq
    zero = jnp.zeros((pair, 128), BF16)
    zero_half = jnp.zeros((seq, 128), BF16)

    def by_head(block):
        return jnp.concatenate([jnp.where(lane, block, zero), jnp.where(lane, zero, block)], 0)

    def packed(block):
        return jnp.where(near, block[:seq], block[seq:])

    def spread(block):
        return jnp.concatenate([jnp.where(near, block, zero_half), jnp.where(near, zero_half, block)], 0)

    blocks = []
    for b in range(pool // 2):
        for j in range(width // 128):
            blocks.append((slice(b * pair, (b + 1) * pair), slice(j * 128, (j + 1) * 128)))
    group = 8
    for first in range(0, len(blocks), group):
        some = blocks[first : first + group]
        score = [dot(by_head(k_s[at, cols]), q_s[at, cols], (1, 1)) * head_scale for at, cols in some]
        grads = [dot(by_head(v_s[at, cols]), c_s[at, cols], (1, 1)) for at, cols in some]
        probs, back = [], []
        for block in range(len(some)):
            probs.append([])
            back.append([])
            for h in range(2):
                of_head = slice(h * pair, (h + 1) * pair)
                s = packed(score[block][of_head])
                e = jnp.exp(s - jnp.max(s, 0, keepdims=True))
                p = e * (1.0 / jnp.sum(e, 0, keepdims=True))
                g = packed(grads[block][of_head])
                d = p * (g - jnp.sum(g * p, 0, keepdims=True)) * head_scale
                probs[-1].append(spread(p.astype(BF16)))
                back[-1].append(spread(d.astype(BF16)))
        for block, (at, cols) in enumerate(some):
            b = at.start // pair
            count = jnp.where(near[:1], counts[2 * b], counts[2 * b + 1])
            context = dot(by_head(v_s[at, cols]), jnp.concatenate(probs[block], 0), (0, 0))
            left_ref[1, cols, at] = (context * count).astype(BF16)
            right_ref[0, at, cols] = dot(jnp.concatenate(back[block], 0), by_head(k_s[at, cols]), (0, 0)).astype(BF16)
            right_ref[1, at, cols] = dot(jnp.concatenate(back[block], 1), by_head(q_s[at, cols]), (1, 0)).astype(BF16)
            right_ref[2, at, cols] = dot(jnp.concatenate(probs[block], 1), by_head(c_s[at, cols]), (1, 0)).astype(BF16)


def local_part(sample_ids, tokens, cotangent, weights):
    pool, seq, width = tokens.shape
    rows = pool * seq
    return pl.pallas_call(
        local_kernel,
        out_shape=(
            jax.ShapeDtypeStruct((2, width, rows), BF16),
            jax.ShapeDtypeStruct((4, rows, width), BF16),
        ),
        in_specs=[pl.BlockSpec(memory_space=ANY)] * 4,
        out_specs=(pl.BlockSpec(memory_space=VMEM), pl.BlockSpec(memory_space=VMEM)),
        scratch_shapes=[
            SMEM(sample_ids.shape, jnp.int32),
            VMEM(tokens.shape, BF16),
            VMEM(weights.shape, BF16),
        ]
        + [VMEM((rows, width), BF16)] * 4
        + [pltpu.SemaphoreType.DMA((6 + pool,))],
        compiler_params=pltpu.CompilerParams(vmem_limit_bytes=32 << 20),
        cost_estimate=pl.CostEstimate(flops=2 * 4 * rows * width * width, bytes_accessed=4 << 20, transcendentals=rows * width),
        name="local",
    )(*[pltpu.with_memory_space_constraint(x, pltpu.HBM) for x in (sample_ids, tokens, cotangent, weights)])


def ring_leg(me, total, stride, size, carry):
    place = lax.rem(me // stride, size)
    down = lax.rem(me + jnp.where(place == 0, (size - 1) * stride, total - stride), total)
    up = lax.rem(me + jnp.where(place == size - 1, total - (size - 1) * stride, stride), total)
    if carry:
        down = jnp.where(place == size - 2, lax.rem(me + (size - 1) * stride, total), down)
        up = jnp.where(place == size - 3, lax.rem(me + total - (size - 1) * stride, total), up)
    return down, up


def jump_leg(me, total, jump):
    return lax.rem(me + jump, total), lax.rem(me + total - jump, total)


def snake_place(z):
    return jnp.where(lax.rem(z, 2) == 1, (z + 1) // 2, lax.rem(8 - z // 2, 8))


def snake_at(place):
    return jnp.where(place == 0, 0, jnp.where(place < 5, 2 * place - 1, 16 - 2 * place))


def detour(total, level):
    if total == 256:
        if level in (1, 3):
            return 4, [partial(ring_leg, total=total, stride=2**level, size=4, carry=leg == 1) for leg in range(3)]
        if level == 5:
            return 2, [partial(jump_leg, total=total, jump=jump) for jump in (160, 160, 224)]
        if level == 6:
            return 4, [partial(jump_leg, total=total, jump=jump) for jump in (160, 160)]
    if total == 8:
        if level == 0:
            return 4, [partial(ring_leg, total=total, stride=1, size=4, carry=leg == 1) for leg in range(3)]
        if level == 1:
            return 4, [partial(jump_leg, total=total, jump=jump) for jump in (5, 5)]
    return 0, []


def exchange_kernel(
    sizes,
    level,
    left_ref,
    right_ref,
    w_hbm,
    r_hbm,
    new_w_hbm,
    new_r_hbm,
    rms_ref,
    w_v,
    r_v,
    grad,
    mine,
    sent,
    got_t,
    got_s,
    out_w,
    out_r,
    square,
    parts,
    w_sem,
    r_sem,
    send_sem,
    recv_sem,
    ow_sem,
    or_sem,
    part_send,
    part_recv,
    rms_s,
    rms_sem,
    relay=None,
    leg_send=None,
    leg_recv=None,
):
    distance = 2**level
    total = 1
    for size in sizes:
        total *= size
    width = w_hbm.shape[-1]
    per = width // ROWS
    chunks = 4 * per
    proj_scale = width**-0.5
    mutual = (2 * distance) % total == 0
    me = lax.axis_index("node")
    ahead = lax.rem(me + distance, total)
    behind = lax.rem(me + total - distance, total)
    away, legs = detour(total, level)
    paths = [leg(me) for leg in legs]
    near = chunks - away
    items = 2 * near
    hops = 2 * away * len(legs)

    groups = []
    strides = []
    stride = 1
    first = 0
    for size in reversed(sizes):
        place = lax.rem(me // stride, size)
        base = me - place * stride
        snake = size == 8 and distance < stride
        if snake:
            place = snake_place(place)
            others = [base + snake_at(lax.rem(place + d, size)) * stride for d in (1, size - 1)]
        else:
            others = [base + lax.rem(place + d, size) * stride for d in range(1, size)]
        places = [lax.rem(place + d, size) for d in range(1, size)]
        groups.append((first, size, place, others, places, snake))
        strides.append(stride)
        first += size
        stride *= size

    barrier = pltpu.get_barrier_semaphore()
    count = 1
    pl.semaphore_signal(barrier, inc=1, device_id=(behind,), device_id_type=pl.DeviceIdType.MESH)
    for _, source in paths:
        pl.semaphore_signal(barrier, inc=1, device_id=(source,), device_id_type=pl.DeviceIdType.MESH)
        count += 1
    for _, _, _, others, _, _ in groups:
        for other in others:
            pl.semaphore_signal(barrier, inc=1, device_id=(other,), device_id_type=pl.DeviceIdType.MESH)
            count += 1

    def at(chunk):
        return chunk // per, pl.ds(pl.multiple_of(lax.rem(chunk, per) * ROWS, ROWS), ROWS)

    def load_r(m):
        return pltpu.make_async_copy(r_hbm.at[m], r_v.at[m], r_sem.at[m])

    load_w = pltpu.make_async_copy(w_hbm, w_v, w_sem)

    for m in range(4):
        load_r(m).start()
    load_w.start()

    square[...] = jnp.zeros_like(square)

    def compute(chunk):
        m, rows = at(chunk)
        g = dot(left_ref[m // 3, rows, :], right_ref[m], (1, 0)) * proj_scale
        grad[m, rows, :] = g
        mine[m, rows, :] = (r_v[m, rows, :].astype(F32) + g).astype(BF16)
        square[...] += jnp.sum((g * g).reshape(ROWS // 8, 8, width), 0)

    def send(item):
        m, rows = at(jnp.where(item < near, item, item - near + away))

        def copy(source, target):
            return pltpu.make_async_remote_copy(
                src_ref=source.at[m, rows],
                dst_ref=target.at[m, rows],
                send_sem=send_sem.at[lax.rem(item, WINDOW)],
                recv_sem=recv_sem.at[item],
                device_id=(ahead,),
                device_id_type=pl.DeviceIdType.MESH,
            )

        return copy

    early, late = ((w_v, got_s), (mine, got_t)) if mutual else ((mine, got_t), (sent, got_s))

    def hop(phase, leg, j):
        m, rows = at((near + j, j)[phase])
        index = (phase * len(legs) + leg) * away + j
        mine_at, got_at = [((mine, got_t), (sent, got_s))[phase][k].at[m, rows] for k in range(2)]
        slot = [relay.at[(phase * (len(legs) - 1) + k) * away + j] for k in range(len(legs) - 1)]
        return pltpu.make_async_remote_copy(
            src_ref=mine_at if leg == 0 else slot[leg - 1],
            dst_ref=got_at if leg == len(legs) - 1 else slot[leg],
            send_sem=leg_send.at[lax.rem(index, RELAYS)],
            recv_sem=leg_recv.at[index],
            device_id=(paths[leg][0],),
            device_id_type=pl.DeviceIdType.MESH,
        )

    def write_r(chunk):
        m, rows = at(chunk)
        return pltpu.make_async_copy(out_r.at[m, rows], new_r_hbm.at[m, rows], or_sem)

    def write_w(chunk):
        m, rows = at(chunk)
        return pltpu.make_async_copy(out_w.at[m, rows], new_w_hbm.at[m, rows], ow_sem)

    def on_tracked(chunk):
        m, rows = at(chunk)
        tracker = 0.5 * (mine[m, rows, :].astype(F32) + got_t[m, rows, :].astype(F32))
        w = w_v[m, rows, :].astype(F32)
        if mutual:
            theirs = (got_s[m, rows, :].astype(F32) - STEP_RATE * tracker).astype(BF16).astype(F32)
            out_w[m, rows, :] = (0.5 * w + 0.5 * theirs - 0.5 * STEP_RATE * tracker).astype(BF16)
        else:
            sent[m, rows, :] = (w - STEP_RATE * tracker).astype(BF16)
        out_r[m, rows, :] = (tracker - grad[m, rows, :]).astype(BF16)
        write_r(chunk).start()
        if mutual:
            write_w(chunk).start()

    def on_sent(chunk):
        m, rows = at(chunk)
        tracker = 0.5 * (mine[m, rows, :].astype(F32) + got_t[m, rows, :].astype(F32))
        w = w_v[m, rows, :].astype(F32)
        out_w[m, rows, :] = (0.5 * w + 0.5 * got_s[m, rows, :].astype(F32) - 0.5 * STEP_RATE * tracker).astype(BF16)
        write_w(chunk).start()

    def part_copy(device, slot, sem):
        return pltpu.make_async_remote_copy(
            src_ref=parts.at[slot],
            dst_ref=parts.at[slot],
            send_sem=part_send.at[sem],
            recv_sem=part_recv.at[slot],
            device_id=(device,),
            device_id_type=pl.DeviceIdType.MESH,
        )

    def part_moves(k, turn):
        start, size, place, others, places, snake = groups[k]
        if not snake:
            return [(others[d], start + place, d) for d in range(size - 1)], [start + p for p in places]
        held = [start + lax.rem(place + d, size) for d in range(size)]
        sends = [(others[0], held[-turn % size], 0)]
        arrivals = [held[-turn - 1]]
        if turn < (size - 1) // 2:
            sends.append((others[-1], held[turn], 1))
            arrivals.append(held[turn + 1])
        return sends, arrivals

    def loaded(k):
        return strides[k] <= distance < strides[k] * groups[k][1]

    turns = []
    tick = -(-(chunks - 1) // BURST) + 1
    last = max(k for k in range(len(groups)) if loaded(k) or (distance == 1 and k == 1))
    for k in [k for k in range(len(groups)) if k != last] + [last]:
        if groups[k][1] > 1:
            for turn in range(groups[k][1] // 2 if groups[k][5] else 1):
                turns.append((tick, k, turn))
                tick += 4 if distance == 1 else 2
    last_tick = max(tick, items + max(WINDOW, LAG + 1 if away else 0))

    def fold(k):
        start, size = groups[k][:2]
        value = parts[start]
        for n in range(1, size):
            value = value + parts[start + n]
        return value

    def end_part(k, turn):
        sends, arrivals = part_moves(k, turn)
        for slot in arrivals:
            part_copy(me, slot, 0).wait_recv()
        for device, slot, sem in sends:
            part_copy(device, slot, sem).wait_send()

    def next_part(index):
        if index:
            end_part(*turns[index - 1][1:])
        if index == len(turns):
            value = fold(turns[-1][1])
            mean = jnp.sum(jnp.sum(value, 1, keepdims=True), 0, keepdims=True) / (total * 4 * width * width)
            rms_s[0] = jnp.sqrt(jnp.broadcast_to(mean, (8, 128)))[0, 0]
            rms_copy().start()
        elif turns[index][2] == 0:
            if index:
                value = fold(turns[index - 1][1])
            else:
                value = square[:, :128]
                for lanes in range(1, width // 128):
                    value = value + square[:, lanes * 128 : (lanes + 1) * 128]
            k = turns[index][1]
            parts[groups[k][0] + groups[k][2]] = value

    def start_part(index):
        for device, slot, sem in part_moves(*turns[index][1:])[0]:
            part_copy(device, slot, sem).start()

    def rms_copy():
        return pltpu.make_async_copy(rms_s, rms_ref, rms_sem)

    def order(k):
        if not away:
            return k
        early_k = jnp.where(lax.rem(k, 2) == 0, k // 2, near + k // 2)
        return jnp.where(k < 2 * away, early_k, k - away)

    if mutual:
        load_w.wait()
    load_r(0).wait()
    if not mutual:
        compute(jnp.int32(0))
    pl.semaphore_wait(barrier, count)
    for m in range(1, 4):
        load_r(m).wait()
    skip = 0 if mutual else 1

    def begun(n):
        return jnp.where(n <= 0, 0, jnp.minimum(hops, (n * hops) // items + jnp.minimum(n, LEAD)))

    def hops_at(n, act):
        def one(index, carry):
            for phase in range(2):
                for leg in range(len(legs)):
                    start = (phase * len(legs) + leg) * away

                    @pl.when(jnp.logical_and(index >= start, index < start + away))
                    def _(phase=phase, leg=leg, start=start):
                        act(phase, leg, index - start)

            return carry

        lax.fori_loop(begun(n), begun(n + 1), one, 0)

    def start_hop(phase, leg, j):
        @pl.when((phase * len(legs) + leg) * away + j >= RELAYS)
        def _():
            hop(phase, leg, j).wait_send()

        if leg:
            hop(phase, leg - 1, j).wait_recv()
        hop(phase, leg, j).start()

    def end_hop(phase, leg, j):
        if leg == len(legs) - 1:
            hop(phase, leg, j).wait_recv()
            if phase == 0:
                on_tracked(near + j)
            else:
                on_sent(j)

    def step(n, carry):
        @pl.when(n < items)
        def _():
            @pl.when(n >= WINDOW)
            def _():
                send(n - WINDOW)(*early).wait_send()

            @pl.when(n < near)
            def _():
                send(n)(*early).start()

            @pl.when(n >= near)
            def _():
                send(n)(*late).start()

        if away:
            hops_at(n - 1, start_hop)

        @pl.when(n <= chunks // BURST)
        def _():
            def some(k, carry):
                compute(order(k))
                return carry

            lax.fori_loop(n * BURST + skip, jnp.minimum((n + 1) * BURST + skip, chunks), some, 0)

        for index, (tick, _, _) in enumerate(turns):

            @pl.when(n == tick)
            def _(index=index):
                next_part(index)

        got = n - WINDOW

        @pl.when(jnp.logical_and(got >= 0, got < near))
        def _():
            if not mutual:
                @pl.when(got == 0)
                def _():
                    load_w.wait()

            send(got)(*early).wait_recv()
            if not mutual:
                on_tracked(got)

        @pl.when(jnp.logical_and(got >= near, got < items))
        def _():
            send(got)(*late).wait_recv()
            if mutual:
                on_tracked(got - near)
            else:
                on_sent(got - near + away)

        if away:
            hops_at(n - 1 - LAG, end_hop)

        for index, (tick, _, _) in enumerate(turns):

            @pl.when(n == tick)
            def _(index=index):
                start_part(index)

        return carry

    lax.fori_loop(0, last_tick, step, 0)
    next_part(len(turns))
    def settle(n, carry):
        send(n)(*late).wait_send()
        return carry

    lax.fori_loop(items - WINDOW, items, settle, 0)
    for index in range(max(0, hops - RELAYS), hops):
        hop(index // (len(legs) * away), index // away % len(legs), index % away).wait_send()
    pltpu.make_async_copy(out_r, new_r_hbm, or_sem).wait()
    pltpu.make_async_copy(out_w, new_w_hbm, ow_sem).wait()
    rms_copy().wait()


def len_bits(sizes):
    return sum(size.bit_length() - 1 for size in sizes)


def exchange_part(sizes, level, left, right, weights, residue):
    shape = weights.shape
    whole = (shape, BF16)
    chunks = 4 * (shape[-1] // ROWS)
    places = sum(sizes)
    away, legs = detour(2 ** len_bits(sizes), level)
    dma = pltpu.SemaphoreType.DMA
    return pl.pallas_call(
        partial(exchange_kernel, sizes, level),
        out_shape=(
            jax.ShapeDtypeStruct(shape, BF16),
            jax.ShapeDtypeStruct(shape, BF16),
            jax.ShapeDtypeStruct((1,), F32),
        ),
        in_specs=[pl.BlockSpec(memory_space=VMEM)] * 2 + [pl.BlockSpec(memory_space=ANY)] * 2,
        out_specs=(pl.BlockSpec(memory_space=ANY),) * 3,
        scratch_shapes=[
            VMEM(*whole),
            VMEM(*whole),
            VMEM(shape, F32),
            VMEM(*whole),
            VMEM(*whole),
            VMEM(*whole),
            VMEM(*whole),
            VMEM(*whole),
            VMEM(*whole),
            VMEM((8, shape[-1]), F32),
            VMEM((places, 8, 128), F32),
            dma,
            dma((4,)),
            dma((WINDOW,)),
            dma((2 * chunks,)),
            dma,
            dma,
            dma((max(sizes),)),
            dma((places,)),
            SMEM((1,), F32),
            dma,
        ]
        + (
            [
                VMEM((2 * (len(legs) - 1) * away, ROWS, shape[-1]), BF16),
                dma((RELAYS,)),
                dma((2 * len(legs) * away,)),
            ]
            if away
            else []
        ),
        compiler_params=pltpu.CompilerParams(
            collective_id=level, has_side_effects=True, vmem_limit_bytes=40 << 20
        ),
        name=f"exchange_{level}",
    )(left, right, weights, residue)


def per_device(sizes, levels, round_index, sample_ids, token_pool, cotangent_pool, weights, residue):
    left, right = local_part(sample_ids, token_pool[0], cotangent_pool[0], weights[0])
    new_weights, new_residue, rms = lax.switch(
        round_index[0] & (levels - 1) if levels == 8 else lax.rem(round_index[0], levels),
        [partial(exchange_part, sizes, level) for level in range(levels)],
        left,
        right,
        weights[0],
        residue[0],
    )
    return new_weights[None], new_residue[None], rms.reshape(())


def solution(mesh):
    nodes = mesh.shape["node"]
    sizes = {256: (8, 4, 4, 2), 16: (2, 2, 2, 2), 8: (2, 1, 4, 1), 4: (1, 1, 2, 2)}[nodes]
    levels = nodes.bit_length() - 1
    split = (P(), P("node", None)) + (P("node", None, None, None),) * 4
    return jax.shard_map(
        partial(per_device, sizes, levels),
        mesh=mesh,
        in_specs=split,
        out_specs=(P("node", None, None, None), P("node", None, None, None), P()),
        check_vma=False,
    )
```

```python
from functools import partial

import jax
import jax.numpy as jnp
from jax import lax
from jax.experimental import pallas as pl
from jax.experimental.pallas import tpu as pltpu
from jax.sharding import PartitionSpec as P

HEAD_DIM = 64
EPSILON = 1e-06
STEP_RATE = 0.1
ROWS = 128
WINDOW = 6
LAG = 4
LEVEL_WITH_LEAD = 5
RELAYS = 8
BURST = 4

F32, BF16 = jnp.float32, jnp.bfloat16
VMEM, SMEM, ANY = pltpu.VMEM, pltpu.SMEM, pl.ANY


def dot(a, b, contract):
    return lax.dot_general(a, b, ((contract[:1], contract[1:]), ((), ())), preferred_element_type=F32)


def local_kernel(
    ids_hbm, token_hbm, cot_hbm, w_hbm, left_ref, right_ref, ids_ref, token_ref, w_ref, q_s, k_s, v_s, c_s, sems
):
    pool, seq, width = token_hbm.shape
    rows = pool * seq
    proj_scale = width**-0.5
    head_scale = HEAD_DIM**-0.5
    loads = [
        pltpu.make_async_copy(ids_hbm, ids_ref, sems.at[0]),
        pltpu.make_async_copy(token_hbm, token_ref, sems.at[1]),
    ]
    loads += [pltpu.make_async_copy(w_hbm.at[m], w_ref.at[m], sems.at[2 + m]) for m in range(4)]
    loads += [
        pltpu.make_async_copy(cot_hbm.at[image], right_ref.at[3, pl.ds(image * seq, seq)], sems.at[6 + image])
        for image in range(pool)
    ]
    for load in loads:
        load.start()
    loads[0].wait()
    counts = []
    for image in range(pool):
        n = jnp.int32(0)
        for b in range(ids_ref.shape[1]):
            n = n + (ids_ref[0, b] == image).astype(jnp.int32)
        counts.append(n.astype(F32))

    loads[1].wait()
    x = token_ref[...].reshape(rows, width).astype(F32)
    centered = x - jnp.mean(x, -1, keepdims=True)
    variance = jnp.mean(centered * centered, -1, keepdims=True)
    normed = (centered * lax.rsqrt(variance + EPSILON)).astype(BF16)
    left_ref[0] = normed.T
    for which, out in enumerate((q_s, k_s, v_s)):
        loads[2 + which].wait()
        out[...] = (dot(normed, w_ref[which], (1, 0)) * proj_scale).astype(BF16)
    loads[5].wait()
    for load in loads[6:]:
        load.wait()
    cg = dot(right_ref[3], w_ref[3], (1, 1))
    for image in range(pool):
        at = slice(image * seq, (image + 1) * seq)
        c_s[at] = (cg[at] * (proj_scale * counts[image])).astype(BF16)

    pair = 2 * seq
    lane = lax.broadcasted_iota(jnp.int32, (pair, 128), 1) < HEAD_DIM
    near = lax.broadcasted_iota(jnp.int32, (seq, 128), 1) < seq
    zero = jnp.zeros((pair, 128), BF16)
    zero_half = jnp.zeros((seq, 128), BF16)

    def by_head(block):
        return jnp.concatenate([jnp.where(lane, block, zero), jnp.where(lane, zero, block)], 0)

    def packed(block):
        return jnp.where(near, block[:seq], block[seq:])

    def spread(block):
        return jnp.concatenate([jnp.where(near, block, zero_half), jnp.where(near, zero_half, block)], 0)

    blocks = []
    for b in range(pool // 2):
        for j in range(width // 128):
            blocks.append((slice(b * pair, (b + 1) * pair), slice(j * 128, (j + 1) * 128)))
    group = 8
    for first in range(0, len(blocks), group):
        some = blocks[first : first + group]
        score = [dot(by_head(k_s[at, cols]), q_s[at, cols], (1, 1)) * head_scale for at, cols in some]
        grads = [dot(by_head(v_s[at, cols]), c_s[at, cols], (1, 1)) for at, cols in some]
        probs, back = [], []
        for block in range(len(some)):
            probs.append([])
            back.append([])
            for h in range(2):
                of_head = slice(h * pair, (h + 1) * pair)
                s = packed(score[block][of_head])
                e = jnp.exp(s - jnp.max(s, 0, keepdims=True))
                p = e * (1.0 / jnp.sum(e, 0, keepdims=True))
                g = packed(grads[block][of_head])
                d = p * (g - jnp.sum(g * p, 0, keepdims=True)) * head_scale
                probs[-1].append(spread(p.astype(BF16)))
                back[-1].append(spread(d.astype(BF16)))
        for block, (at, cols) in enumerate(some):
            b = at.start // pair
            count = jnp.where(near[:1], counts[2 * b], counts[2 * b + 1])
            context = dot(by_head(v_s[at, cols]), jnp.concatenate(probs[block], 0), (0, 0))
            left_ref[1, cols, at] = (context * count).astype(BF16)
            right_ref[0, at, cols] = dot(jnp.concatenate(back[block], 0), by_head(k_s[at, cols]), (0, 0)).astype(BF16)
            right_ref[1, at, cols] = dot(jnp.concatenate(back[block], 1), by_head(q_s[at, cols]), (1, 0)).astype(BF16)
            right_ref[2, at, cols] = dot(jnp.concatenate(probs[block], 1), by_head(c_s[at, cols]), (1, 0)).astype(BF16)


def local_part(sample_ids, tokens, cotangent, weights):
    pool, seq, width = tokens.shape
    rows = pool * seq
    return pl.pallas_call(
        local_kernel,
        out_shape=(
            jax.ShapeDtypeStruct((2, width, rows), BF16),
            jax.ShapeDtypeStruct((4, rows, width), BF16),
        ),
        in_specs=[pl.BlockSpec(memory_space=ANY)] * 4,
        out_specs=(pl.BlockSpec(memory_space=VMEM), pl.BlockSpec(memory_space=VMEM)),
        scratch_shapes=[
            SMEM(sample_ids.shape, jnp.int32),
            VMEM(tokens.shape, BF16),
            VMEM(weights.shape, BF16),
        ]
        + [VMEM((rows, width), BF16)] * 4
        + [pltpu.SemaphoreType.DMA((6 + pool,))],
        compiler_params=pltpu.CompilerParams(vmem_limit_bytes=32 << 20),
        cost_estimate=pl.CostEstimate(flops=2 * 4 * rows * width * width, bytes_accessed=4 << 20, transcendentals=rows * width),
        name="local",
    )(*[pltpu.with_memory_space_constraint(x, pltpu.HBM) for x in (sample_ids, tokens, cotangent, weights)])


def ring_leg(me, total, stride, size, carry):
    place = lax.rem(me // stride, size)
    down = lax.rem(me + jnp.where(place == 0, (size - 1) * stride, total - stride), total)
    up = lax.rem(me + jnp.where(place == size - 1, total - (size - 1) * stride, stride), total)
    if carry:
        down = jnp.where(place == size - 2, lax.rem(me + (size - 1) * stride, total), down)
        up = jnp.where(place == size - 3, lax.rem(me + total - (size - 1) * stride, total), up)
    return down, up


def jump_leg(me, total, jump):
    return lax.rem(me + jump, total), lax.rem(me + total - jump, total)


def snake_place(z):
    return jnp.where(lax.rem(z, 2) == 1, (z + 1) // 2, lax.rem(8 - z // 2, 8))


def snake_at(place):
    return jnp.where(place == 0, 0, jnp.where(place < 5, 2 * place - 1, 16 - 2 * place))


def detour(total, level):
    if total == 256:
        if level in (1, 3):
            return 4, [partial(ring_leg, total=total, stride=2**level, size=4, carry=leg == 1) for leg in range(3)]
        if level == 5:
            return 2, [partial(jump_leg, total=total, jump=jump) for jump in (160, 160, 224)]
        if level == 6:
            return 4, [partial(jump_leg, total=total, jump=jump) for jump in (160, 160)]
    if total == 8:
        if level == 0:
            return 4, [partial(ring_leg, total=total, stride=1, size=4, carry=leg == 1) for leg in range(3)]
        if level == 1:
            return 4, [partial(jump_leg, total=total, jump=jump) for jump in (5, 5)]
    return 0, []


def exchange_kernel(
    sizes,
    level,
    left_ref,
    right_ref,
    w_hbm,
    r_hbm,
    new_w_hbm,
    new_r_hbm,
    rms_ref,
    w_v,
    r_v,
    grad,
    mine,
    sent,
    got_t,
    got_s,
    out_w,
    out_r,
    square,
    parts,
    w_sem,
    r_sem,
    send_sem,
    recv_sem,
    ow_sem,
    or_sem,
    part_send,
    part_recv,
    rms_s,
    rms_sem,
    relay=None,
    leg_send=None,
    leg_recv=None,
):
    distance = 2**level
    total = 1
    for size in sizes:
        total *= size
    width = w_hbm.shape[-1]
    per = width // ROWS
    chunks = 4 * per
    proj_scale = width**-0.5
    mutual = (2 * distance) % total == 0
    me = lax.axis_index("node")
    ahead = lax.rem(me + distance, total)
    behind = lax.rem(me + total - distance, total)
    away, legs = detour(total, level)
    paths = [leg(me) for leg in legs]
    near = chunks - away
    items = 2 * near
    hops = 2 * away * len(legs)

    groups = []
    strides = []
    stride = 1
    first = 0
    for size in reversed(sizes):
        place = lax.rem(me // stride, size)
        base = me - place * stride
        snake = size == 8 and distance < stride
        if snake:
            place = snake_place(place)
            others = [base + snake_at(lax.rem(place + d, size)) * stride for d in (1, size - 1)]
        else:
            others = [base + lax.rem(place + d, size) * stride for d in range(1, size)]
        places = [lax.rem(place + d, size) for d in range(1, size)]
        groups.append((first, size, place, others, places, snake))
        strides.append(stride)
        first += size
        stride *= size

    barrier = pltpu.get_barrier_semaphore()
    count = 1
    pl.semaphore_signal(barrier, inc=1, device_id=(behind,), device_id_type=pl.DeviceIdType.MESH)
    for _, source in paths:
        pl.semaphore_signal(barrier, inc=1, device_id=(source,), device_id_type=pl.DeviceIdType.MESH)
        count += 1
    for _, _, _, others, _, _ in groups:
        for other in others:
            pl.semaphore_signal(barrier, inc=1, device_id=(other,), device_id_type=pl.DeviceIdType.MESH)
            count += 1

    def at(chunk):
        return chunk // per, pl.ds(pl.multiple_of(lax.rem(chunk, per) * ROWS, ROWS), ROWS)

    def load_r(m):
        return pltpu.make_async_copy(r_hbm.at[m], r_v.at[m], r_sem.at[m])

    load_w = pltpu.make_async_copy(w_hbm, w_v, w_sem)

    for m in range(4):
        load_r(m).start()
    load_w.start()

    square[...] = jnp.zeros_like(square)

    def compute(chunk):
        m, rows = at(chunk)
        g = dot(left_ref[m // 3, rows, :], right_ref[m], (1, 0)) * proj_scale
        grad[m, rows, :] = g
        mine[m, rows, :] = (r_v[m, rows, :].astype(F32) + g).astype(BF16)
        square[...] += jnp.sum((g * g).reshape(ROWS // 8, 8, width), 0)

    def send(item):
        m, rows = at(jnp.where(item < near, item, item - near + away))

        def copy(source, target):
            return pltpu.make_async_remote_copy(
                src_ref=source.at[m, rows],
                dst_ref=target.at[m, rows],
                send_sem=send_sem.at[lax.rem(item, WINDOW)],
                recv_sem=recv_sem.at[item],
                device_id=(ahead,),
                device_id_type=pl.DeviceIdType.MESH,
            )

        return copy

    early, late = ((w_v, got_s), (mine, got_t)) if mutual else ((mine, got_t), (sent, got_s))

    def hop(phase, leg, j):
        m, rows = at((near + j, j)[phase])
        index = (phase * len(legs) + leg) * away + j
        mine_at, got_at = [((mine, got_t), (sent, got_s))[phase][k].at[m, rows] for k in range(2)]
        slot = [relay.at[(phase * (len(legs) - 1) + k) * away + j] for k in range(len(legs) - 1)]
        return pltpu.make_async_remote_copy(
            src_ref=mine_at if leg == 0 else slot[leg - 1],
            dst_ref=got_at if leg == len(legs) - 1 else slot[leg],
            send_sem=leg_send.at[lax.rem(index, RELAYS)],
            recv_sem=leg_recv.at[index],
            device_id=(paths[leg][0],),
            device_id_type=pl.DeviceIdType.MESH,
        )

    def write_r(chunk):
        m, rows = at(chunk)
        return pltpu.make_async_copy(out_r.at[m, rows], new_r_hbm.at[m, rows], or_sem)

    def write_w(chunk):
        m, rows = at(chunk)
        return pltpu.make_async_copy(out_w.at[m, rows], new_w_hbm.at[m, rows], ow_sem)

    def on_tracked(chunk):
        m, rows = at(chunk)
        tracker = 0.5 * (mine[m, rows, :].astype(F32) + got_t[m, rows, :].astype(F32))
        w = w_v[m, rows, :].astype(F32)
        if mutual:
            theirs = (got_s[m, rows, :].astype(F32) - STEP_RATE * tracker).astype(BF16).astype(F32)
            out_w[m, rows, :] = (0.5 * w + 0.5 * theirs - 0.5 * STEP_RATE * tracker).astype(BF16)
        else:
            sent[m, rows, :] = (w - STEP_RATE * tracker).astype(BF16)
        out_r[m, rows, :] = (tracker - grad[m, rows, :]).astype(BF16)
        write_r(chunk).start()
        if mutual:
            write_w(chunk).start()

    def on_sent(chunk):
        m, rows = at(chunk)
        tracker = 0.5 * (mine[m, rows, :].astype(F32) + got_t[m, rows, :].astype(F32))
        w = w_v[m, rows, :].astype(F32)
        out_w[m, rows, :] = (0.5 * w + 0.5 * got_s[m, rows, :].astype(F32) - 0.5 * STEP_RATE * tracker).astype(BF16)
        write_w(chunk).start()

    def part_copy(device, slot, sem):
        return pltpu.make_async_remote_copy(
            src_ref=parts.at[slot],
            dst_ref=parts.at[slot],
            send_sem=part_send.at[sem],
            recv_sem=part_recv.at[slot],
            device_id=(device,),
            device_id_type=pl.DeviceIdType.MESH,
        )

    def part_moves(k, turn):
        start, size, place, others, places, snake = groups[k]
        if not snake:
            return [(others[d], start + place, d) for d in range(size - 1)], [start + p for p in places]
        held = [start + lax.rem(place + d, size) for d in range(size)]
        sends = [(others[0], held[-turn % size], 0)]
        arrivals = [held[-turn - 1]]
        if turn < (size - 1) // 2:
            sends.append((others[-1], held[turn], 1))
            arrivals.append(held[turn + 1])
        return sends, arrivals

    def loaded(k):
        return strides[k] <= distance < strides[k] * groups[k][1]

    turns = []
    tick = -(-(chunks - 1) // BURST) + 1
    last = max(k for k in range(len(groups)) if loaded(k) or (distance == 1 and k == 1))
    for k in [k for k in range(len(groups)) if k != last] + [last]:
        if groups[k][1] > 1:
            for turn in range(groups[k][1] // 2 if groups[k][5] else 1):
                turns.append((tick, k, turn))
                tick += 4 if distance == 1 else 2
    last_tick = max(tick, items + max(WINDOW, LAG + 1 if away else 0))

    def fold(k):
        start, size = groups[k][:2]
        value = parts[start]
        for n in range(1, size):
            value = value + parts[start + n]
        return value

    def end_part(k, turn):
        sends, arrivals = part_moves(k, turn)
        for slot in arrivals:
            part_copy(me, slot, 0).wait_recv()
        for device, slot, sem in sends:
            part_copy(device, slot, sem).wait_send()

    def next_part(index):
        if index:
            end_part(*turns[index - 1][1:])
        if index == len(turns):
            value = fold(turns[-1][1])
            mean = jnp.sum(jnp.sum(value, 1, keepdims=True), 0, keepdims=True) / (total * 4 * width * width)
            rms_s[0] = jnp.sqrt(jnp.broadcast_to(mean, (8, 128)))[0, 0]
            rms_copy().start()
        elif turns[index][2] == 0:
            if index:
                value = fold(turns[index - 1][1])
            else:
                value = square[:, :128]
                for lanes in range(1, width // 128):
                    value = value + square[:, lanes * 128 : (lanes + 1) * 128]
            k = turns[index][1]
            parts[groups[k][0] + groups[k][2]] = value

    def start_part(index):
        for device, slot, sem in part_moves(*turns[index][1:])[0]:
            part_copy(device, slot, sem).start()

    def rms_copy():
        return pltpu.make_async_copy(rms_s, rms_ref, rms_sem)

    def order(k):
        if not away:
            return k
        early_k = jnp.where(lax.rem(k, 2) == 0, k // 2, near + k // 2)
        return jnp.where(k < 2 * away, early_k, k - away)

    if mutual:
        load_w.wait()
    load_r(0).wait()
    if not mutual:
        compute(jnp.int32(0))
    pl.semaphore_wait(barrier, count)
    for m in range(1, 4):
        load_r(m).wait()
    skip = 0 if mutual else 1

    def begun(n):
        return jnp.where(n <= 0, 0, jnp.minimum(hops, (n * hops) // items + jnp.minimum(n, 1 if level == LEVEL_WITH_LEAD else 0)))

    def hops_at(n, act):
        def one(index, carry):
            for phase in range(2):
                for leg in range(len(legs)):
                    start = (phase * len(legs) + leg) * away

                    @pl.when(jnp.logical_and(index >= start, index < start + away))
                    def _(phase=phase, leg=leg, start=start):
                        act(phase, leg, index - start)

            return carry

        lax.fori_loop(begun(n), begun(n + 1), one, 0)

    def start_hop(phase, leg, j):
        @pl.when((phase * len(legs) + leg) * away + j >= RELAYS)
        def _():
            hop(phase, leg, j).wait_send()

        if leg:
            hop(phase, leg - 1, j).wait_recv()
        hop(phase, leg, j).start()

    def end_hop(phase, leg, j):
        if leg == len(legs) - 1:
            hop(phase, leg, j).wait_recv()
            if phase == 0:
                on_tracked(near + j)
            else:
                on_sent(j)

    def step(n, carry):
        @pl.when(n < items)
        def _():
            @pl.when(n >= WINDOW)
            def _():
                send(n - WINDOW)(*early).wait_send()

            @pl.when(n < near)
            def _():
                send(n)(*early).start()

            @pl.when(n >= near)
            def _():
                send(n)(*late).start()

        if away:
            hops_at(n - 1, start_hop)

        @pl.when(n <= chunks // BURST)
        def _():
            def some(k, carry):
                compute(order(k))
                return carry

            lax.fori_loop(n * BURST + skip, jnp.minimum((n + 1) * BURST + skip, chunks), some, 0)

        for index, (tick, _, _) in enumerate(turns):

            @pl.when(n == tick)
            def _(index=index):
                next_part(index)

        got = n - WINDOW

        @pl.when(jnp.logical_and(got >= 0, got < near))
        def _():
            if not mutual:
                @pl.when(got == 0)
                def _():
                    load_w.wait()

            send(got)(*early).wait_recv()
            if not mutual:
                on_tracked(got)

        @pl.when(jnp.logical_and(got >= near, got < items))
        def _():
            send(got)(*late).wait_recv()
            if mutual:
                on_tracked(got - near)
            else:
                on_sent(got - near + away)

        if away:
            hops_at(n - 1 - LAG, end_hop)

        for index, (tick, _, _) in enumerate(turns):

            @pl.when(n == tick)
            def _(index=index):
                start_part(index)

        return carry

    lax.fori_loop(0, last_tick, step, 0)
    next_part(len(turns))
    def settle(n, carry):
        send(n)(*late).wait_send()
        return carry

    lax.fori_loop(items - WINDOW, items, settle, 0)
    for index in range(max(0, hops - RELAYS), hops):
        hop(index // (len(legs) * away), index // away % len(legs), index % away).wait_send()
    pltpu.make_async_copy(out_r, new_r_hbm, or_sem).wait()
    pltpu.make_async_copy(out_w, new_w_hbm, ow_sem).wait()
    rms_copy().wait()


def len_bits(sizes):
    return sum(size.bit_length() - 1 for size in sizes)


def exchange_part(sizes, level, left, right, weights, residue):
    shape = weights.shape
    whole = (shape, BF16)
    chunks = 4 * (shape[-1] // ROWS)
    places = sum(sizes)
    away, legs = detour(2 ** len_bits(sizes), level)
    dma = pltpu.SemaphoreType.DMA
    return pl.pallas_call(
        partial(exchange_kernel, sizes, level),
        out_shape=(
            jax.ShapeDtypeStruct(shape, BF16),
            jax.ShapeDtypeStruct(shape, BF16),
            jax.ShapeDtypeStruct((1,), F32),
        ),
        in_specs=[pl.BlockSpec(memory_space=VMEM)] * 2 + [pl.BlockSpec(memory_space=ANY)] * 2,
        out_specs=(pl.BlockSpec(memory_space=ANY),) * 3,
        scratch_shapes=[
            VMEM(*whole),
            VMEM(*whole),
            VMEM(shape, F32),
            VMEM(*whole),
            VMEM(*whole),
            VMEM(*whole),
            VMEM(*whole),
            VMEM(*whole),
            VMEM(*whole),
            VMEM((8, shape[-1]), F32),
            VMEM((places, 8, 128), F32),
            dma,
            dma((4,)),
            dma((WINDOW,)),
            dma((2 * chunks,)),
            dma,
            dma,
            dma((max(sizes),)),
            dma((places,)),
            SMEM((1,), F32),
            dma,
        ]
        + (
            [
                VMEM((2 * (len(legs) - 1) * away, ROWS, shape[-1]), BF16),
                dma((RELAYS,)),
                dma((2 * len(legs) * away,)),
            ]
            if away
            else []
        ),
        compiler_params=pltpu.CompilerParams(
            collective_id=level, has_side_effects=True, vmem_limit_bytes=40 << 20
        ),
        name=f"exchange_{level}",
    )(left, right, weights, residue)


def per_device(sizes, levels, round_index, sample_ids, token_pool, cotangent_pool, weights, residue):
    left, right = local_part(sample_ids, token_pool[0], cotangent_pool[0], weights[0])
    new_weights, new_residue, rms = lax.switch(
        round_index[0] & (levels - 1) if levels == 8 else lax.rem(round_index[0], levels),
        [partial(exchange_part, sizes, level) for level in range(levels)],
        left,
        right,
        weights[0],
        residue[0],
    )
    return new_weights[None], new_residue[None], rms.reshape(())


def solution(mesh):
    nodes = mesh.shape["node"]
    sizes = {256: (8, 4, 4, 2), 16: (2, 2, 2, 2), 8: (2, 1, 4, 1), 4: (1, 1, 2, 2)}[nodes]
    levels = nodes.bit_length() - 1
    split = (P(), P("node", None)) + (P("node", None, None, None),) * 4
    return jax.shard_map(
        partial(per_device, sizes, levels),
        mesh=mesh,
        in_specs=split,
        out_specs=(P("node", None, None, None), P("node", None, None, None), P()),
        check_vma=False,
    )
```
